128 devices in a mesh: leaf: 16 (over x, z), sub: 8 (over y, core).
Axes of the slice: x: 4, y: 4, z: 4, core: 2. Of those that a mesh axis runs over, the one named last changes fastest.
Arguments:
- vectors: bfloat16 [64, 655360], P(None, ('leaf', 'sub')), may hold values from -6 to 6
- row_counts: int32 [128], replicated, may hold values from 3072 to 5120, as said below
- tree_slot: int32 [655360], P(('leaf', 'sub')), may hold values from -1 to 524287, as said below
- leaf_inverse: bfloat16 [2048, 256, 256], P(('leaf', 'sub')), may hold values from -0.375 to 0.375
- left_basis: bfloat16 [11, 32, 524288], P(None, None, ('leaf', 'sub')), may hold values from -0.41992188 to 0.41992188
- right_basis: bfloat16 [11, 32, 524288], P(None, None, ('leaf', 'sub')), may hold values from -6 to 6
Outputs:
- applied: bfloat16 [64, 655360], P(None, ('leaf', 'sub'))
The draws below stay inside these ranges and needn't reach their ends.
Inputs may be any that keep to these rules, and one draw needn't show every extreme that they name: The first row_counts[d] of the 5120 slots of owner d are live; the counts sum to 524288. `tree_slot`: live slots hold distinct tree positions covering 0 .. 524287, dead slots hold -1. Tree owner t holds positions t*4096 .. (t+1)*4096 - 1; the live rows of one mesh owner go to one tree owner at most 40 at a time.
All inputs are finite; a program needn't handle non-finite values.
Results may differ from the reference program's by a relative error of at most 0.014.
Values may be sent and summed in bfloat16 or wider, within the bound.
A program may use at most 64 MiB of HBM per device.

```python
import math
import jax
import jax.numpy as jnp
from jax import lax

VECS = 64
LEAF = 256
RANK = 32
ROWS_DEV = 4096
MESH_CAP = 5120
LEVELS = 11
TOTAL = 524288
N_LEAF = 16
N_SUB = 8
DEVICES = 128


def mesh_plan(key):
    base = jax.random.fold_in(key, 7)
    devices = N_LEAF * N_SUB
    quarter = ROWS_DEV // 4
    k_pair, k_extra, k_owner, k_local = jax.random.split(base, 4)
    pairing = jax.random.permutation(k_pair, devices).astype(jnp.int32)
    half = devices // 2
    extra = jax.random.randint(k_extra, (half,), 0, quarter + 1).astype(jnp.int32)
    extra = extra.at[0].set(quarter)
    delta = jnp.zeros((devices,), jnp.int32).at[pairing[:half]].set(extra).at[pairing[half:]].set(-extra)
    counts = ROWS_DEV + delta
    owner_perm = jax.random.permutation(k_owner, devices).astype(jnp.int32)
    local_perm = jax.vmap(lambda k: jax.random.permutation(k, ROWS_DEV).astype(jnp.int32))(jax.random.split(k_local, devices))
    offsets = jnp.cumsum(counts) - counts
    slot = jnp.arange(devices * MESH_CAP, dtype=jnp.int32)
    owner = slot // MESH_CAP
    within = slot % MESH_CAP
    live = within < counts[owner]
    glob = jnp.where(live, offsets[owner] + within, 0)
    dest = owner_perm[glob % devices]
    place = local_perm[dest, glob // devices]
    tree = jnp.where(live, dest * ROWS_DEV + place, -1).astype(jnp.int32)
    return (counts, tree)


def draw_row_counts(key, part):
    return mesh_plan(key)[0]


def draw_tree_slot(key, part):
    return mesh_plan(key)[1]


def levels(stream_key, extent, cuts, low, largest):
    gain, own = 1.0, jax.random.fold_in(stream_key, 6)
    for axis_at, blocks in cuts:
        steps = jnp.exp(jax.random.uniform(jax.random.fold_in(own, axis_at), (blocks,), jnp.float32, low / len(cuts), largest / len(cuts)))
        gain = gain * jnp.repeat(steps, extent[axis_at] // blocks).reshape([-1 if axis == axis_at else 1 for axis in range(len(extent))])
    return gain


def noise(own_key, dims, spread, reach, cuts=(), held_as=jnp.bfloat16):
    level = levels(own_key, dims, cuts, -0.22, 0.18) if cuts else 1.0
    array = jax.random.normal(own_key, dims, jnp.float32) * spread * level
    return jnp.minimum(jnp.maximum(array, -reach), reach).astype(held_as)


def setup_inputs(seed: int = 0) -> dict:
    streams_of = jax.random.split(jax.random.key(seed), 7)
    return {
        "vectors": noise(streams_of[0], (VECS, DEVICES * MESH_CAP), 1.0, 6.0, ((1, 128),)),
        "row_counts": draw_row_counts(jax.random.fold_in(streams_of[6], 71), 0),
        "tree_slot": draw_tree_slot(jax.random.fold_in(streams_of[6], 71), 0),
        "leaf_inverse": noise(streams_of[3], (TOTAL // LEAF, LEAF, LEAF), LEAF ** -0.5, 0.375, ((0, 128),)),
        "left_basis": noise(streams_of[4], (LEVELS, RANK, TOTAL), 0.07, 0.41992188, ((2, 128),)),
        "right_basis": noise(streams_of[5], (LEVELS, RANK, TOTAL), 1.0, 6.0, ((2, 128),)),
    }


def reference(vectors, row_counts, tree_slot, leaf_inverse, left_basis, right_basis):
    devices = N_LEAF * N_SUB
    total = ROWS_DEV * devices
    slot = jnp.arange(devices * MESH_CAP, dtype=jnp.int32)
    owner = slot // MESH_CAP
    within = slot % MESH_CAP
    live = (within < row_counts[owner]) & (tree_slot >= 0)
    target = jnp.where(live, tree_slot, total).astype(jnp.int32)
    tree = jnp.zeros((VECS, total), jnp.bfloat16).at[:, target].set(vectors, mode='drop')
    blocks = tree.reshape(VECS, total // LEAF, LEAF).astype(jnp.float32)
    field = jnp.einsum('lij,vlj->vli', leaf_inverse.astype(jnp.float32), blocks, precision=lax.Precision.HIGHEST).reshape(VECS, total)
    for level in range(LEVELS):
        size = LEAF * 2 ** level
        nodes = total // size
        rounded = field.astype(jnp.bfloat16).astype(jnp.float32)
        right = right_basis[level].reshape(RANK, nodes, size).astype(jnp.float32)
        coeff = jnp.einsum('rns,vns->nrv', right, rounded.reshape(VECS, nodes, size), precision=lax.Precision.HIGHEST) / math.sqrt(size)
        partner = coeff.reshape(nodes // 2, 2, RANK, VECS)[:, ::-1].reshape(nodes, RANK, VECS)
        partner = partner.astype(jnp.bfloat16).astype(jnp.float32)
        left = left_basis[level].reshape(RANK, nodes, size).astype(jnp.float32)
        field = field - jnp.einsum('rns,nrv->vns', left, partner, precision=lax.Precision.HIGHEST).reshape(VECS, total)
    done = field.astype(jnp.bfloat16)
    picked = done[:, jnp.minimum(target, total - 1)]
    return jnp.where(live[None, :], picked, jnp.zeros_like(picked)).astype(jnp.bfloat16)
```

```python
import functools
import math

import jax
import jax.numpy as jnp
from jax import lax
from jax.experimental import pallas as pl
from jax.experimental.pallas import tpu as pltpu
from jax.sharding import PartitionSpec as P

DEV = 128
PEER = 40
HALF = 20
BLOCK = 24
ROWS = 4096
SLOTS = 5120
VECS = 64
LEAF = 256
RANK = 32
LOCAL = 4
CROSS = 7
F32 = jnp.float32
BF16 = jnp.bfloat16
I32 = jnp.int32
VMEM = pl.BlockSpec(memory_space=pltpu.VMEM)
SMEM = pl.BlockSpec(memory_space=pltpu.SMEM)
NT = (((1,), (1,)), ((), ()))
MESH = pl.DeviceIdType.MESH


def my_index():
    return lax.axis_index("leaf") * 8 + lax.axis_index("sub")


def iota(shape, dim):
    return lax.broadcasted_iota(I32, shape, dim)


def dot_nt(a, b):
    return lax.dot_general(a, b, NT, preferred_element_type=F32)


def dot(a, b):
    return jnp.dot(a, b, preferred_element_type=F32)


def bucket_row(owner, rank):
    return jnp.where(rank < HALF, owner * BLOCK + rank, DEV * BLOCK + owner * BLOCK + rank - HALF)


def live_slots(counts, slots):
    place = iota((40, 128), 0) * 128 + iota((40, 128), 1)
    return (place < counts[my_index()]) & (slots >= 0)


def route(counts, slots_ref, rank_ref):
    slots = slots_ref[...]
    live = live_slots(counts, slots)
    owner = jnp.where(live, slots >> 12, DEV)
    high = ((slots & 4095) >> 6).astype(F32)
    low = (slots & 63).astype(F32)
    ids = iota((DEV, 128), 0)
    before = jnp.where(iota((128, 256), 0) < iota((128, 256), 1), 1.0, 0.0).astype(BF16)
    base = jnp.zeros((DEV, 128), F32)
    for a in range(40):
        hit = ids == owner[a : a + 1, :]
        earlier = dot(jnp.where(hit, 1.0, 0.0).astype(BF16), before)
        rank_ref[a : a + 1, :] = jnp.sum(jnp.where(hit, base + earlier[:, :128], 0.0), axis=0, keepdims=True)
        base = base + earlier[:, 128:]
    ranks = rank_ref[...].astype(I32)
    r64 = iota((64, 128), 0)
    lane = iota((64, 128), 1).astype(F32)
    total = jnp.zeros((DEV, 256), F32)
    for a in range(40):
        hit = jnp.where(ids == owner[a : a + 1, :], 1.0, 0.0).astype(BF16)
        match = r64 == ranks[a : a + 1, :]
        table = jnp.concatenate(
            [
                jnp.where(match, float(a), 0.0),
                jnp.where(match, lane, 0.0),
                jnp.where(match, high[a : a + 1, :], 0.0),
                jnp.where(match, low[a : a + 1, :], 0.0),
            ],
            axis=0,
        ).astype(BF16)
        total = total + dot_nt(hit, table)
    return live, owner, ranks, base, total


def bucket_kernel(counts, slots_ref, vec, out, flat, pick_v, pick, rank_ref, x, stage, sem):
    live, owner, ranks, base, total = route(counts, slots_ref, rank_ref)
    flat[...] = jnp.where(live, bucket_row(owner, ranks), 0)
    both = total[:, :128].astype(I32)
    source = both * 128 + pltpu.roll(both, 64, 1)
    lane128 = iota((DEV, 128), 1)
    pick_v[...] = jnp.where(lane128 < PEER, source, 0)
    copy = pltpu.make_async_copy(pick_v, pick, sem)
    copy.start()
    filled = lane128.astype(F32) < base
    position = total[:, 128:]
    stage[pl.ds(20, DEV, stride=BLOCK), :] = jnp.where(filled, position, 64.0)
    stage[pl.ds(21, DEV, stride=BLOCK), :] = pltpu.roll(position, 64, 1)
    stage[pl.ds(22, DEV, stride=BLOCK), :] = jnp.zeros((DEV, 128), F32)
    stage[pl.ds(23, DEV, stride=BLOCK), :] = jnp.zeros((DEV, 128), F32)
    for a in range(40):
        part = vec[:, a * 128 : (a + 1) * 128].astype(F32)
        x[a * 128 : (a + 1) * 128, :] = jnp.concatenate([part, part], axis=0).T
    copy.wait()
    gather_buckets(pick, x, stage, out)


def gather_buckets(pick, x, stage, out):
    left = iota((1, 128), 1) < VECS

    def four(c, carry):
        for u in range(4):
            t = c * 4 + u
            for r in range(HALF):
                one = x[pl.ds(pick[t, r], 1), :]
                two = x[pl.ds(pick[t, r + HALF], 1), :]
                stage[pl.ds(t * BLOCK + r, 1), :] = jnp.where(left, one, two)
        for u in range(4):
            t = c * 4 + u
            out[t] = stage[pl.ds(pl.multiple_of(t * BLOCK, 8), BLOCK), :].astype(BF16)
        return carry

    lax.fori_loop(0, DEV // 4, four, 0)


def spread(arrived, y):
    def eight(c, carry):
        for u in range(8):
            t = c * 8 + u
            rows = arrived[t].astype(F32)
            at = pl.multiple_of(t * BLOCK, 8)
            y[pl.ds(at, BLOCK), :] = rows
            y[pl.ds(pl.multiple_of(DEV * BLOCK + at, 8), BLOCK), :] = pltpu.roll(rows, 64, 1)
        return carry

    lax.fori_loop(0, DEV // 8, eight, 0)


def all_to_all_kernel(src, dst, send_sem, recv_sem, own_sem):
    me = my_index()
    own = pltpu.make_async_copy(src.at[me], dst.at[me], own_sem)
    own.start()

    def copy_to(i):
        peer = lax.rem(me + i, DEV)
        return pltpu.make_async_remote_copy(
            src_ref=src.at[peer],
            dst_ref=dst.at[me],
            send_sem=send_sem.at[i],
            recv_sem=recv_sem.at[me],
            device_id={"leaf": peer // 8, "sub": lax.rem(peer, 8)},
            device_id_type=MESH,
        )

    def start(i, carry):
        copy_to(i).start()
        return carry

    lax.fori_loop(1, DEV, start, 0)

    def finish(i, carry):
        source = lax.rem(me + i, DEV)
        copy_to(i).wait_send()
        pltpu.make_async_copy(dst.at[source], dst.at[source], recv_sem.at[source]).wait()
        return carry

    lax.fori_loop(1, DEV, finish, 0)
    own.wait()


def all_to_all(blocks):
    return pl.pallas_call(
        all_to_all_kernel,
        out_shape=jax.ShapeDtypeStruct((DEV, BLOCK, 128), BF16),
        in_specs=[VMEM],
        out_specs=VMEM,
        scratch_shapes=[
            pltpu.SemaphoreType.DMA((DEV,)),
            pltpu.SemaphoreType.DMA((DEV,)),
            pltpu.SemaphoreType.DMA,
        ],
        compiler_params=pltpu.CompilerParams(has_side_effects=True),
        name="exchange",
    )(blocks)


def tree_kernel(arrived, inverse, left, right, field, reduced, back, inv_v, inv, y, rows, sem):
    spread(arrived, y)
    high = y[pl.ds(20, DEV, stride=BLOCK), :]
    low = y[pl.ds(21, DEV, stride=BLOCK), :]
    lane128 = iota((DEV, 128), 1)
    place = high.astype(I32) * 64 + low.astype(I32)
    back[...] = jnp.where(lane128 < PEER, jnp.minimum(place, ROWS - 1), 0)
    high_t = high.T
    low_t = low.T
    ids = iota((64, 128), 0).astype(F32)
    owner = iota((64, 128), 1).astype(F32)
    total = jnp.zeros((64, 128), F32)
    for r in range(PEER):
        hit = jnp.where(ids == high_t[r : r + 1, :], 1.0, 0.0).astype(BF16)
        match = ids == low_t[r : r + 1, :]
        table = jnp.concatenate([jnp.where(match, owner, 0.0), jnp.where(match, float(r), 0.0)], axis=0).astype(BF16)
        total = total + dot_nt(hit, table)
    whole = total.astype(I32)
    inv_v[...] = jnp.where(iota((64, 128), 1) < 64, bucket_row(whole, pltpu.roll(whole, 64, 1)), 0)
    copy = pltpu.make_async_copy(inv_v, inv, sem)
    copy.start()
    copy.wait()

    def some(c, carry):
        for u in range(128):
            rows[pl.ds(c * 128 + u, 1), :] = y[pl.ds(inv[c * 2 + u // 64, u % 64], 1), :]
        return carry

    lax.fori_loop(0, ROWS // 128, some, 0)

    def leaf(l, carry):
        at = pl.multiple_of(l * LEAF, LEAF)
        block = rows[pl.ds(at, LEAF), :].T[:VECS].astype(BF16)
        field[:, pl.ds(at, LEAF)] = dot_nt(block, inverse[l])
        return carry

    lax.fori_loop(0, ROWS // LEAF, leaf, 0)
    for level in range(LOCAL):
        size = LEAF * 2**level
        nodes = ROWS // size
        scale = 1.0 / math.sqrt(size)

        def pair(m, carry):
            at = [pl.multiple_of(m * 2 * size, size), pl.multiple_of(m * 2 * size + size, size)]
            coeff = [
                (
                    dot_nt(field[:, pl.ds(s, size)].astype(BF16), right[level, :, pl.ds(s, size)]) * scale
                ).astype(BF16)
                for s in at
            ]
            for n in range(2):
                field[:, pl.ds(at[n], size)] -= dot(coeff[1 - n], left[level, :, pl.ds(at[n], size)])
            return carry

        lax.fori_loop(0, nodes // 2, pair, 0, unroll=True)
    acc = jnp.zeros((VECS + CROSS * RANK, CROSS * RANK), F32)
    for c in range(4):
        at = slice(c * 1024, (c + 1) * 1024)
        lhs = jnp.concatenate(
            [field[:, at].astype(BF16), left[LOCAL:, :, at].reshape(CROSS * RANK, 1024)], axis=0
        )
        acc = acc + dot_nt(lhs, right[LOCAL:, :, at].reshape(CROSS * RANK, 1024))
    reduced[...] = acc


def cross_kernel(mine, out, v_send, g_send, v_a, g_a, v_b, g_b, v_c, g_c, v_d, g_d, send_v, send_g, recv_v, recv_g):
    leaf, sub = lax.axis_index("leaf"), lax.axis_index("sub")
    x, z, y, core = leaf // 4, lax.rem(leaf, 4), sub // 2, lax.rem(sub, 2)
    scale = [1.0 / math.sqrt(ROWS * 2**k) for k in range(CROSS)]

    def block(k):
        return slice((CROSS - 1 - k) * RANK, (CROSS - k) * RANK)

    def above(k):
        return slice(0, (CROSS - 1 - k) * RANK)

    def rows_of(j):
        return slice((5 - j) * RANK, (6 - j) * RANK)

    def exchange(phase, v, g, v_buf, g_buf, peers, me, target):
        copies = []
        for i in range(1, peers):
            other = lax.rem(me + i, peers)
            for n, (src, dst, s_sem, r_sem) in enumerate(
                ((v, v_buf, send_v, recv_v), (g, g_buf, send_g, recv_g))
            ):
                copy = pltpu.make_async_remote_copy(
                    src_ref=src,
                    dst_ref=dst.at[me],
                    send_sem=s_sem.at[phase, i],
                    recv_sem=r_sem.at[phase, me],
                    device_id=target(other),
                    device_id_type=MESH,
                )
                copy.start()
                copies.append(copy)
        for copy in copies:
            copy.wait_send()
        for i in range(1, peers):
            other = lax.rem(me + i, peers)
            for dst, r_sem in ((v_buf, recv_v), (g_buf, recv_g)):
                pltpu.make_async_copy(dst.at[other], dst.at[other], r_sem.at[phase, other]).wait()

    def merge(k, va, vb, ga, gb):
        pa = (vb[:, block(k)] * scale[k]).astype(BF16)
        pb = (va[:, block(k)] * scale[k]).astype(BF16)
        if k == CROSS - 1:
            return pa, pb, None
        p2 = jnp.concatenate([pa, pb], axis=1)
        g2 = jnp.concatenate([ga[rows_of(k), above(k)], gb[rows_of(k), above(k)]], axis=0).astype(BF16)
        return pa, pb, va[:, above(k)] + vb[:, above(k)] - dot(p2, g2)

    def keep(k, p):
        out[:, k * RANK : (k + 1) * RANK] = p

    v_send[...] = jnp.zeros_like(v_send)
    for k in range(CROSS):
        v_send[:, block(k)] = mine[:VECS, k * RANK : (k + 1) * RANK]
    g_send[...] = jnp.zeros_like(g_send)
    for j in range(CROSS - 1):
        for k in range(j + 1, CROSS):
            g_send[rows_of(j), block(k)] = mine[
                VECS + j * RANK : VECS + (j + 1) * RANK, k * RANK : (k + 1) * RANK
            ].astype(BF16)
    v_a[core] = v_send[...]
    g_a[core] = g_send[...]
    exchange(0, v_send, g_send, v_a, g_a, 2, core, lambda c: {"leaf": leaf, "sub": y * 2 + c})
    pa, pb, v = merge(0, v_a[0], v_a[1], g_a[0], g_a[1])
    keep(0, jnp.where(core == 0, pa, pb))
    g = g_a[0].astype(F32) + g_a[1].astype(F32)
    out[:, CROSS * RANK :] = jnp.zeros((VECS, 32), BF16)

    def four(phase, k, v, g, v_buf, g_buf, me, target):
        width, height = v_buf.shape[2], g_buf.shape[1]
        part = jnp.concatenate([v, jnp.zeros((VECS, width), F32)], axis=1)[:, :width]
        v_buf[me] = part
        g_buf[me] = g[:height, : g_buf.shape[2]].astype(BF16)
        exchange(phase, v_buf.at[me], g_buf.at[me], v_buf, g_buf, 4, me, target)
        vs = [v_buf[i] for i in range(4)]
        gs = [g_buf[i].astype(F32) for i in range(4)]
        p0, p1, v01 = merge(k, vs[0], vs[1], gs[0], gs[1])
        p2, p3, v23 = merge(k, vs[2], vs[3], gs[2], gs[3])
        keep(k, jnp.where(me < 2, jnp.where(me == 0, p0, p1), jnp.where(me == 2, p2, p3)))
        g01, g23 = gs[0] + gs[1], gs[2] + gs[3]
        pa, pb, v = merge(k + 1, v01, v23, g01, g23)
        keep(k + 1, jnp.where(me < 2, pa, pb))
        return v, g01 + g23

    v, g = four(1, 1, v, g, v_b, g_b, y, lambda c: {"leaf": leaf, "sub": c * 2 + core})
    v, g = four(2, 3, v, g, v_c, g_c, z, lambda c: {"leaf": x * 4 + c, "sub": sub})
    four(3, 5, v, g, v_d, g_d, x, lambda c: {"leaf": c * 4 + z, "sub": sub})


def finish_kernel(field, partner, left, pick, out, rows, stage):
    for c in range(16):
        at = slice(c * LEAF, (c + 1) * LEAF)
        done = field[:, at] - dot(
            partner[:, : CROSS * RANK], left[LOCAL:, :, at].reshape(CROSS * RANK, LEAF)
        )
        rows[at, :] = jnp.concatenate([done, done], axis=0).T
    for r in range(HALF, BLOCK):
        stage[pl.ds(r, DEV, stride=BLOCK), :] = jnp.zeros((DEV, 128), F32)
    gather_buckets(pick, rows, stage, out)


def output_kernel(counts, slots_ref, flat, returned, out, y, rows):
    spread(returned, y)
    live = jnp.where(live_slots(counts, slots_ref[...]), 1, 0)

    def gather(c, carry):
        for u in range(128):
            rows[pl.ds(c * 128 + u, 1), :] = y[pl.ds(flat[c, u], 1), :]
        return carry

    lax.fori_loop(0, 40, gather, 0)
    for a in range(40):
        part = rows[a * 128 : (a + 1) * 128, :].T[:VECS]
        out[:, a * 128 : (a + 1) * 128] = jnp.where(live[a : a + 1, :] > 0, part, 0.0).astype(BF16)


def body(vectors, row_counts, tree_slot, leaf_inverse, left_basis, right_basis):
    shape = jax.ShapeDtypeStruct
    slots = tree_slot.reshape(40, 128)
    outgoing, flat = pl.pallas_call(
        bucket_kernel,
        out_shape=[shape((DEV, BLOCK, 128), BF16), shape((40, 128), I32)],
        in_specs=[SMEM, VMEM, VMEM],
        out_specs=[VMEM, VMEM],
        scratch_shapes=[
            pltpu.VMEM((DEV, 128), I32),
            pltpu.SMEM((DEV, 128), I32),
            pltpu.VMEM((40, 128), F32),
            pltpu.VMEM((SLOTS, 128), F32),
            pltpu.VMEM((DEV * BLOCK, 128), F32),
            pltpu.SemaphoreType.DMA,
        ],
        name="bucket",
    )(row_counts, slots, vectors)
    arrived = all_to_all(outgoing)
    field, reduced, back = pl.pallas_call(
        tree_kernel,
        out_shape=[
            shape((VECS, ROWS), F32),
            shape((VECS + CROSS * RANK, CROSS * RANK), F32),
            shape((DEV, 128), I32),
        ],
        in_specs=[VMEM] * 4,
        out_specs=[VMEM] * 3,
        scratch_shapes=[
            pltpu.VMEM((64, 128), I32),
            pltpu.SMEM((64, 128), I32),
            pltpu.VMEM((2 * DEV * BLOCK, 128), F32),
            pltpu.VMEM((ROWS, 128), F32),
            pltpu.SemaphoreType.DMA,
        ],
        name="tree",
    )(arrived, leaf_inverse, left_basis, right_basis)
    partner = pl.pallas_call(
        cross_kernel,
        out_shape=shape((VECS, 256), BF16),
        in_specs=[VMEM],
        out_specs=VMEM,
        scratch_shapes=[
            pltpu.VMEM((VECS, 256), F32),
            pltpu.VMEM((192, 256), BF16),
            pltpu.VMEM((2, VECS, 256), F32),
            pltpu.VMEM((2, 192, 256), BF16),
            pltpu.VMEM((4, VECS, 256), F32),
            pltpu.VMEM((4, 160, 256), BF16),
            pltpu.VMEM((4, VECS, 128), F32),
            pltpu.VMEM((4, 96, 128), BF16),
            pltpu.VMEM((4, VECS, 128), F32),
            pltpu.VMEM((4, 32, 128), BF16),
            pltpu.SemaphoreType.DMA((4, 4)),
            pltpu.SemaphoreType.DMA((4, 4)),
            pltpu.SemaphoreType.DMA((4, 4)),
            pltpu.SemaphoreType.DMA((4, 4)),
        ],
        compiler_params=pltpu.CompilerParams(has_side_effects=True),
        name="cross",
    )(reduced)
    outgoing = pl.pallas_call(
        finish_kernel,
        out_shape=shape((DEV, BLOCK, 128), BF16),
        in_specs=[VMEM, VMEM, VMEM, SMEM],
        out_specs=VMEM,
        scratch_shapes=[pltpu.VMEM((ROWS, 128), F32), pltpu.VMEM((DEV * BLOCK, 128), F32)],
        name="finish",
    )(field, partner, left_basis, back)
    returned = all_to_all(outgoing)
    return pl.pallas_call(
        output_kernel,
        out_shape=shape((VECS, SLOTS), BF16),
        in_specs=[SMEM, VMEM, SMEM, VMEM],
        out_specs=VMEM,
        scratch_shapes=[pltpu.VMEM((2 * DEV * BLOCK, 128), F32), pltpu.VMEM((SLOTS, 128), F32)],
        name="output",
    )(row_counts, slots, flat, returned)


def solution(mesh):
    both = ("leaf", "sub")
    return jax.shard_map(
        body,
        mesh=mesh,
        in_specs=(
            P(None, both),
            P(),
            P(both),
            P(both, None, None),
            P(None, None, both),
            P(None, None, both),
        ),
        out_specs=P(None, both),
        check_vma=False,
    )
```

```python
import functools
import math

import jax
import jax.numpy as jnp
from jax import lax
from jax.experimental import pallas as pl
from jax.experimental.pallas import tpu as pltpu
from jax.sharding import PartitionSpec as P

DEV = 128
PEER = 40
HALF = 20
BLOCK = 24
ROWS = 4096
SLOTS = 5120
VECS = 64
LEAF = 256
RANK = 32
LOCAL = 4
CROSS = 7
F32 = jnp.float32
BF16 = jnp.bfloat16
I32 = jnp.int32
VMEM = pl.BlockSpec(memory_space=pltpu.VMEM)
SMEM = pl.BlockSpec(memory_space=pltpu.SMEM)
NT = (((1,), (1,)), ((), ()))
MESH = pl.DeviceIdType.MESH


def my_index():
    return lax.axis_index("leaf") * 8 + lax.axis_index("sub")


def iota(shape, dim):
    return lax.broadcasted_iota(I32, shape, dim)


def dot_nt(a, b):
    return lax.dot_general(a, b, NT, preferred_element_type=F32)


def dot(a, b):
    return jnp.dot(a, b, preferred_element_type=F32)


def bucket_row(owner, rank):
    return jnp.where(rank < HALF, owner * BLOCK + rank, DEV * BLOCK + owner * BLOCK + rank - HALF)


def live_slots(counts, slots):
    place = iota((40, 128), 0) * 128 + iota((40, 128), 1)
    return (place < counts[my_index()]) & (slots >= 0)


def route(counts, slots_ref, rank_ref):
    slots = slots_ref[...]
    live = live_slots(counts, slots)
    owner = jnp.where(live, slots >> 12, DEV)
    high = ((slots & 4095) >> 6).astype(F32)
    low = (slots & 63).astype(F32)
    ids = iota((DEV, 128), 0)
    before = jnp.where(iota((128, 256), 0) < iota((128, 256), 1), 1.0, 0.0).astype(BF16)
    base = jnp.zeros((DEV, 128), F32)
    for a in range(40):
        hit = ids == owner[a : a + 1, :]
        earlier = dot(jnp.where(hit, 1.0, 0.0).astype(BF16), before)
        rank_ref[a : a + 1, :] = jnp.sum(jnp.where(hit, base + earlier[:, :128], 0.0), axis=0, keepdims=True)
        base = base + earlier[:, 128:]
    ranks = rank_ref[...].astype(I32)
    r64 = iota((64, 128), 0)
    lane = iota((64, 128), 1).astype(F32)
    total = jnp.zeros((DEV, 256), F32)
    for a in range(40):
        hit = jnp.where(ids == owner[a : a + 1, :], 1.0, 0.0).astype(BF16)
        match = r64 == ranks[a : a + 1, :]
        table = jnp.concatenate(
            [
                jnp.where(match, float(a), 0.0),
                jnp.where(match, lane, 0.0),
                jnp.where(match, high[a : a + 1, :], 0.0),
                jnp.where(match, low[a : a + 1, :], 0.0),
            ],
            axis=0,
        ).astype(BF16)
        total = total + dot_nt(hit, table)
    return live, owner, ranks, base, total


def device(index):
    return {"leaf": index // 8, "sub": lax.rem(index, 8)}


def enter():
    me = my_index()
    barrier = pltpu.get_barrier_semaphore()

    def signal(i, carry):
        pl.semaphore_signal(barrier, 1, device_id=device(lax.rem(me + i, DEV)), device_id_type=MESH)
        return carry

    lax.fori_loop(1, DEV, signal, 0)


def entered():
    pl.semaphore_wait(pltpu.get_barrier_semaphore(), DEV - 1)


def send_block(src, dst, t, send_sem, recv_sem):
    me = my_index()

    @pl.when(t != me)
    def _():
        pltpu.make_async_remote_copy(
            src_ref=src.at[t],
            dst_ref=dst.at[me],
            send_sem=send_sem,
            recv_sem=recv_sem.at[me],
            device_id=device(t),
            device_id_type=MESH,
        ).start()

    @pl.when(t == me)
    def _():
        pltpu.make_async_copy(src.at[t], dst.at[t], recv_sem.at[t]).start()


def sent(src, send_sem):
    whole = src.at[pl.ds(0, DEV - 1)]
    pltpu.make_async_copy(whole, whole, send_sem).wait()


def gather_and_send(pick, x, stage, src, dst, send_sem, recv_sem):
    left = iota((1, 128), 1) < VECS
    me = my_index()

    def some(c, carry):
        ts = [lax.rem(me + 1 + c * 4 + u, DEV) for u in range(4)]
        for u, t in enumerate(ts):
            for r in range(HALF):
                one = x[pl.ds(pick[t, r], 1), :]
                two = x[pl.ds(pick[t, r + HALF], 1), :]
                stage[u, r : r + 1, :] = jnp.where(left, one, two)
            for r in range(HALF, HALF + 2):
                stage[u, r : r + 1, :] = x[pl.ds(SLOTS + (r - HALF) * DEV + t, 1), :]
            src[t] = stage[u].astype(BF16)
        for t in ts:
            send_block(src, dst, t, send_sem, recv_sem)
        return carry

    lax.fori_loop(0, DEV // 4, some, 0)


def receive(arrived, recv_sem, y):
    me = my_index()

    def some(c, carry):
        for u in range(4):
            t = lax.rem(me + 2 * DEV - 1 - c * 4 - u, DEV)
            pltpu.make_async_copy(arrived.at[t], arrived.at[t], recv_sem.at[t]).wait()
            rows = arrived[t].astype(F32)
            at = pl.multiple_of(t * BLOCK, 8)
            y[pl.ds(at, BLOCK), :] = rows
            y[pl.ds(pl.multiple_of(DEV * BLOCK + at, 8), BLOCK), :] = pltpu.roll(rows, 64, 1)
        return carry

    lax.fori_loop(0, DEV // 4, some, 0)


def block(k):
    return slice((CROSS - 1 - k) * RANK, (CROSS - k) * RANK)


def above(k):
    return slice(0, (CROSS - 1 - k) * RANK)


def rows_of(j):
    return slice((5 - j) * RANK, (6 - j) * RANK)


def place():
    leaf, sub = lax.axis_index("leaf"), lax.axis_index("sub")
    return leaf // 4, lax.rem(leaf, 4), sub // 2, lax.rem(sub, 2)


def group(phase):
    x, z, y, core = place()
    leaf, sub = lax.axis_index("leaf"), lax.axis_index("sub")
    return [
        (2, core, lambda c: {"leaf": leaf, "sub": y * 2 + c}),
        (4, y, lambda c: {"leaf": leaf, "sub": c * 2 + core}),
        (4, z, lambda c: {"leaf": x * 4 + c, "sub": sub}),
        (4, x, lambda c: {"leaf": c * 4 + z, "sub": sub}),
    ][phase]


def share(phase, buf, send_sem, recv_sem, wait=False):
    members, me, target = group(phase)
    for i in range(1, members):
        other = lax.rem(me + i, members)
        copy = pltpu.make_async_remote_copy(
            src_ref=buf.at[me],
            dst_ref=buf.at[me],
            send_sem=send_sem.at[phase, i],
            recv_sem=recv_sem.at[phase, me],
            device_id=target(other),
            device_id_type=MESH,
        )
        if wait:
            copy.wait_send()
            pltpu.make_async_copy(buf.at[other], buf.at[other], recv_sem.at[phase, other]).wait()
        else:
            copy.start()


def kernel(
    counts,
    slots_ref,
    vec,
    inverse_h,
    left_h,
    right_h,
    out,
    inverse,
    left,
    right,
    pick_v,
    pick,
    rank_ref,
    flat_v,
    flat,
    x,
    stage,
    src1,
    dst1,
    src2,
    dst2,
    y,
    inv_v,
    inv,
    back_v,
    back,
    field,
    v_a,
    v_b,
    v_c,
    v_d,
    g_a,
    g_b,
    g_c,
    g_d,
    partner,
    load_sem,
    index_sem,
    send_sem,
    recv1,
    recv2,
    send_v,
    recv_v,
    send_g,
    recv_g,
):
    scale = [1.0 / math.sqrt(ROWS * 2**k) for k in range(CROSS)]
    with jax.named_scope("enter"):
        loads = [
            pltpu.make_async_copy(h, v, load_sem.at[i])
            for i, (h, v) in enumerate(((left_h, left), (right_h, right), (inverse_h, inverse)))
        ]
        for load in loads:
            load.start()
        enter()
    with jax.named_scope("route"):
        live, owner, ranks, base, total = route(counts, slots_ref, rank_ref)
        flat_v[...] = jnp.clip(jnp.where(live, bucket_row(owner, ranks), 0), 0, 2 * DEV * BLOCK - 1)
        both = total[:, :128].astype(I32)
        source = both * 128 + pltpu.roll(both, 64, 1)
        lane128 = iota((DEV, 128), 1)
        pick_v[...] = jnp.clip(jnp.where(lane128 < PEER, source, 0), 0, SLOTS - 1)
        pick_copy = pltpu.make_async_copy(pick_v, pick, index_sem.at[0])
        pick_copy.start()
        flat_copy = pltpu.make_async_copy(flat_v, flat, index_sem.at[1])
        flat_copy.start()
        position = total[:, 128:]
        x[SLOTS : SLOTS + DEV, :] = jnp.where(lane128.astype(F32) < base, position, 64.0)
        x[SLOTS + DEV :, :] = pltpu.roll(position, 64, 1)
    with jax.named_scope("rows"):
        for a in range(40):
            part = vec[:, a * 128 : (a + 1) * 128].astype(F32)
            x[a * 128 : (a + 1) * 128, :] = jnp.concatenate([part, part], axis=0).T
        for u in range(4):
            stage[u] = jnp.zeros((BLOCK, 128), F32)
        pick_copy.wait()
    with jax.named_scope("entered"):
        entered()
    with jax.named_scope("send"):
        gather_and_send(pick, x, stage, src1, dst1, send_sem.at[0], recv1)
    with jax.named_scope("gram"):
        loads[0].wait()
        loads[1].wait()
        gram = jnp.zeros((CROSS * RANK - RANK, CROSS * RANK), F32)
        for c in range(4):
            at = slice(c * 1024, (c + 1) * 1024)
            gram = gram + dot_nt(
                left[LOCAL : LOCAL + 6, :, at].reshape(6 * RANK, 1024),
                right[LOCAL:, :, at].reshape(CROSS * RANK, 1024),
            )
        core = group(0)[1]
        g_a[core] = jnp.zeros((192, 256), BF16)
        for j in range(CROSS - 1):
            for k in range(j + 1, CROSS):
                g_a[core, rows_of(j), block(k)] = gram[
                    j * RANK : (j + 1) * RANK, k * RANK : (k + 1) * RANK
                ].astype(BF16)
        share(0, g_a, send_g, recv_g)
    with jax.named_scope("receive"):
        receive(dst1, recv1, y)
    with jax.named_scope("inv"):
        high = y[pl.ds(20, DEV, stride=BLOCK), :]
        low = y[pl.ds(21, DEV, stride=BLOCK), :]
        spot = high.astype(I32) * 64 + low.astype(I32)
        back_v[...] = jnp.clip(jnp.where(lane128 < PEER, spot, 0), 0, ROWS - 1)
        back_copy = pltpu.make_async_copy(back_v, back, index_sem.at[2])
        back_copy.start()
        high_t = high.T
        low_t = low.T
        ids = iota((64, 128), 0).astype(F32)
        lanes = iota((64, 128), 1).astype(F32)
        found = jnp.zeros((64, 128), F32)
        for r in range(PEER):
            hit = jnp.where(ids == high_t[r : r + 1, :], 1.0, 0.0).astype(BF16)
            match = ids == low_t[r : r + 1, :]
            table = jnp.concatenate(
                [jnp.where(match, lanes, 0.0), jnp.where(match, float(r), 0.0)], axis=0
            ).astype(BF16)
            found = found + dot_nt(hit, table)
        whole = found.astype(I32)
        inv_v[...] = jnp.clip(
            jnp.where(iota((64, 128), 1) < 64, bucket_row(whole, pltpu.roll(whole, 64, 1)), 0),
            0,
            2 * DEV * BLOCK - 1,
        )
        inv_copy = pltpu.make_async_copy(inv_v, inv, index_sem.at[3])
        inv_copy.start()
    with jax.named_scope("gram_y"):
        share(0, g_a, send_g, recv_g, wait=True)
        ysum = g_a[0].astype(F32) + g_a[1].astype(F32)
        g_b[group(1)[1]] = ysum[:160].astype(BF16)
        share(1, g_b, send_g, recv_g)
        inv_copy.wait()
    with jax.named_scope("tree"):

        def some(c, carry):
            for u in range(128):
                x[pl.ds(c * 128 + u, 1), :] = y[pl.ds(inv[c * 2 + u // 64, u % 64], 1), :]
            return carry

        lax.fori_loop(0, ROWS // 128, some, 0)
    with jax.named_scope("leaf"):
        loads[2].wait()

        def leaf(l, carry):
            at = pl.multiple_of(l * LEAF, LEAF)
            rows = x[pl.ds(at, LEAF), :].T[:VECS].astype(BF16)
            field[:, pl.ds(at, LEAF)] = dot_nt(rows, inverse[l])
            return carry

        lax.fori_loop(0, ROWS // LEAF, leaf, 0)
    with jax.named_scope("gram_z"):
        share(1, g_b, send_g, recv_g, wait=True)
        zsum = (g_b[0, :96, :128].astype(F32) + g_b[1, :96, :128].astype(F32)) + (
            g_b[2, :96, :128].astype(F32) + g_b[3, :96, :128].astype(F32)
        )
        g_c[group(2)[1]] = zsum.astype(BF16)
        share(2, g_c, send_g, recv_g)
    with jax.named_scope("local"):
        for level in range(LOCAL):
            size = LEAF * 2**level
            nodes = ROWS // size

            def pair(m, carry):
                at = [pl.multiple_of(m * 2 * size, size), pl.multiple_of(m * 2 * size + size, size)]
                coeff = [
                    (
                        dot_nt(field[:, pl.ds(s, size)].astype(BF16), right[level, :, pl.ds(s, size)])
                        * (1.0 / math.sqrt(size))
                    ).astype(BF16)
                    for s in at
                ]
                for n in range(2):
                    field[:, pl.ds(at[n], size)] -= dot(coeff[1 - n], left[level, :, pl.ds(at[n], size)])
                return carry

            lax.fori_loop(0, nodes // 2, pair, 0, unroll=True)
    with jax.named_scope("gram_x"):
        share(2, g_c, send_g, recv_g, wait=True)
        xsum = (g_c[0, :32].astype(F32) + g_c[1, :32].astype(F32)) + (
            g_c[2, :32].astype(F32) + g_c[3, :32].astype(F32)
        )
        g_d[group(3)[1]] = xsum.astype(BF16)
        share(3, g_d, send_g, recv_g)
    with jax.named_scope("reduce"):
        v = jnp.zeros((VECS, CROSS * RANK), F32)
        for c in range(4):
            at = slice(c * 1024, (c + 1) * 1024)
            v = v + dot_nt(field[:, at].astype(BF16), right[LOCAL:, :, at].reshape(CROSS * RANK, 1024))

    def merge(k, va, vb, ga, gb):
        pa = (vb[:, block(k)] * scale[k]).astype(BF16)
        pb = (va[:, block(k)] * scale[k]).astype(BF16)
        if k == CROSS - 1:
            return pa, pb, None
        p2 = jnp.concatenate([pa, pb], axis=1)
        g2 = jnp.concatenate([ga[rows_of(k), above(k)], gb[rows_of(k), above(k)]], axis=0).astype(BF16)
        return pa, pb, va[:, above(k)] + vb[:, above(k)] - dot(p2, g2)

    def keep(k, p):
        partner[:, k * RANK : (k + 1) * RANK] = p

    with jax.named_scope("cross_core"):
        core = group(0)[1]
        v_a[core] = jnp.zeros((VECS, 256), F32)
        for k in range(CROSS):
            v_a[core, :, block(k)] = v[:, k * RANK : (k + 1) * RANK]
        share(0, v_a, send_v, recv_v)
        share(0, v_a, send_v, recv_v, wait=True)
        pa, pb, v = merge(0, v_a[0], v_a[1], g_a[0], g_a[1])
        keep(0, jnp.where(core == 0, pa, pb))

    def four(phase, k, v, v_buf, g_buf):
        me = group(phase)[1]
        width = v_buf.shape[2]
        v_buf[me] = jnp.concatenate([v, jnp.zeros((VECS, width), F32)], axis=1)[:, :width].astype(BF16)
        share(phase, v_buf, send_v, recv_v)
        share(phase, v_buf, send_v, recv_v, wait=True)
        vs = [v_buf[i].astype(F32) for i in range(4)]
        gs = [g_buf[i].astype(F32) for i in range(4)]
        p0, p1, v01 = merge(k, vs[0], vs[1], gs[0], gs[1])
        p2, p3, v23 = merge(k, vs[2], vs[3], gs[2], gs[3])
        keep(k, jnp.where(me < 2, jnp.where(me == 0, p0, p1), jnp.where(me == 2, p2, p3)))
        pa, pb, v = merge(k + 1, v01, v23, gs[0] + gs[1], gs[2] + gs[3])
        keep(k + 1, jnp.where(me < 2, pa, pb))
        return v

    with jax.named_scope("cross_y"):
        v = four(1, 1, v, v_b, g_b)
    with jax.named_scope("cross_z"):
        v = four(2, 3, v, v_c, g_c)
    with jax.named_scope("cross_x"):
        share(3, g_d, send_g, recv_g, wait=True)
        four(3, 5, v, v_d, g_d)
    with jax.named_scope("finish"):
        for c in range(16):
            at = slice(c * LEAF, (c + 1) * LEAF)
            done = field[:, at] - dot(
                partner[:, : CROSS * RANK], left[LOCAL:, :, at].reshape(CROSS * RANK, LEAF)
            )
            x[at, :] = jnp.concatenate([done, done], axis=0).T
        back_copy.wait()
        sent(src1, send_sem.at[0])
    with jax.named_scope("send_back"):
        gather_and_send(back, x, stage, src2, dst2, send_sem.at[1], recv2)
    with jax.named_scope("receive_back"):
        flat_copy.wait()
        receive(dst2, recv2, y)
    with jax.named_scope("output"):
        alive = jnp.where(live_slots(counts, slots_ref[...]), 1, 0)

        def pull(c, carry):
            for u in range(128):
                x[pl.ds(c * 128 + u, 1), :] = y[pl.ds(flat[c, u], 1), :]
            return carry

        lax.fori_loop(0, 40, pull, 0)
        for a in range(40):
            part = x[a * 128 : (a + 1) * 128, :].T[:VECS]
            out[:, a * 128 : (a + 1) * 128] = jnp.where(alive[a : a + 1, :] > 0, part, 0.0).astype(BF16)
        sent(src2, send_sem.at[1])


def body(vectors, row_counts, tree_slot, leaf_inverse, left_basis, right_basis):
    anywhere = pl.BlockSpec(memory_space=pl.ANY)
    dma = pltpu.SemaphoreType.DMA
    blocks = pltpu.VMEM((DEV, BLOCK, 128), BF16)
    return pl.pallas_call(
        kernel,
        out_shape=jax.ShapeDtypeStruct((VECS, SLOTS), BF16),
        in_specs=[SMEM, VMEM, VMEM, anywhere, anywhere, anywhere],
        out_specs=VMEM,
        scratch_shapes=[
            pltpu.VMEM(leaf_inverse.shape, BF16),
            pltpu.VMEM(left_basis.shape, BF16),
            pltpu.VMEM(right_basis.shape, BF16),
            pltpu.VMEM((DEV, 128), I32),
            pltpu.SMEM((DEV, 128), I32),
            pltpu.VMEM((40, 128), F32),
            pltpu.VMEM((40, 128), I32),
            pltpu.SMEM((40, 128), I32),
            pltpu.VMEM((SLOTS + 2 * DEV, 128), F32),
            pltpu.VMEM((4, BLOCK, 128), F32),
            blocks,
            blocks,
            blocks,
            blocks,
            pltpu.VMEM((2 * DEV * BLOCK, 128), F32),
            pltpu.VMEM((64, 128), I32),
            pltpu.SMEM((64, 128), I32),
            pltpu.VMEM((DEV, 128), I32),
            pltpu.SMEM((DEV, 128), I32),
            pltpu.VMEM((VECS, ROWS), F32),
            pltpu.VMEM((2, VECS, 256), F32),
            pltpu.VMEM((4, VECS, 256), BF16),
            pltpu.VMEM((4, VECS, 128), BF16),
            pltpu.VMEM((4, VECS, 128), BF16),
            pltpu.VMEM((2, 192, 256), BF16),
            pltpu.VMEM((4, 160, 256), BF16),
            pltpu.VMEM((4, 96, 128), BF16),
            pltpu.VMEM((4, 32, 128), BF16),
            pltpu.VMEM((VECS, 256), BF16),
            dma((3,)),
            dma((4,)),
            dma((2,)),
            dma((DEV,)),
            dma((DEV,)),
            dma((4, 4)),
            dma((4, 4)),
            dma((4, 4)),
            dma((4, 4)),
        ],
        compiler_params=pltpu.CompilerParams(collective_id=0, has_side_effects=True),
        name="apply",
    )(row_counts, tree_slot.reshape(40, 128), vectors, leaf_inverse, left_basis, right_basis)


def solution(mesh):
    both = ("leaf", "sub")
    return jax.shard_map(
        body,
        mesh=mesh,
        in_specs=(
            P(None, both),
            P(),
            P(both),
            P(both, None, None),
            P(None, None, both),
            P(None, None, both),
        ),
        out_specs=P(None, both),
        check_vma=False,
    )
```

```python
import functools
import math

import jax
import jax.numpy as jnp
from jax import lax
from jax.experimental import pallas as pl
from jax.experimental.pallas import tpu as pltpu
from jax.sharding import PartitionSpec as P

DEV = 128
PEER = 40
HALF = 20
BLOCK = 24
ROWS = 4096
SLOTS = 5120
VECS = 64
LEAF = 256
RANK = 32
LOCAL = 4
CROSS = 7
F32 = jnp.float32
BF16 = jnp.bfloat16
I32 = jnp.int32
VMEM = pl.BlockSpec(memory_space=pltpu.VMEM)
SMEM = pl.BlockSpec(memory_space=pltpu.SMEM)
NT = (((1,), (1,)), ((), ()))
MESH = pl.DeviceIdType.MESH


def my_index():
    return lax.axis_index("leaf") * 8 + lax.axis_index("sub")


def iota(shape, dim):
    return lax.broadcasted_iota(I32, shape, dim)


def dot_nt(a, b):
    return lax.dot_general(a, b, NT, preferred_element_type=F32)


def dot(a, b):
    return jnp.dot(a, b, preferred_element_type=F32)


def bucket_row(owner, rank):
    return jnp.where(rank < HALF, owner * BLOCK + rank, DEV * BLOCK + owner * BLOCK + rank - HALF)


def live_slots(counts, slots):
    place = iota((40, 128), 0) * 128 + iota((40, 128), 1)
    return (place < counts[my_index()]) & (slots >= 0)


def route(counts, slots_ref, rank_ref):
    slots = slots_ref[...]
    live = live_slots(counts, slots)
    owner = jnp.where(live, slots >> 12, DEV)
    high = ((slots & 4095) >> 6).astype(F32)
    low = (slots & 63).astype(F32)
    ids = iota((DEV, 128), 0)
    before = jnp.where(iota((128, 256), 0) < iota((128, 256), 1), 1.0, 0.0).astype(BF16)
    base = jnp.zeros((DEV, 128), F32)
    for a in range(40):
        hit = ids == owner[a : a + 1, :]
        earlier = dot(jnp.where(hit, 1.0, 0.0).astype(BF16), before)
        rank_ref[a : a + 1, :] = jnp.sum(jnp.where(hit, base + earlier[:, :128], 0.0), axis=0, keepdims=True)
        base = base + earlier[:, 128:]
    ranks = rank_ref[...].astype(I32)
    r64 = iota((64, 128), 0)
    lane = iota((64, 128), 1).astype(F32)
    total = jnp.zeros((DEV, 256), F32)
    for a in range(40):
        hit = jnp.where(ids == owner[a : a + 1, :], 1.0, 0.0).astype(BF16)
        match = r64 == ranks[a : a + 1, :]
        table = jnp.concatenate(
            [
                jnp.where(match, float(a), 0.0),
                jnp.where(match, lane, 0.0),
                jnp.where(match, high[a : a + 1, :], 0.0),
                jnp.where(match, low[a : a + 1, :], 0.0),
            ],
            axis=0,
        ).astype(BF16)
        total = total + dot_nt(hit, table)
    return live, owner, ranks, base, total


def far_first():
    def hops(c):
        return sum(min(d, 4 - d) for d in c)

    chips = [(i * 29 % 64 // 16, i * 29 % 16 // 4, i * 29 % 4) for i in range(64)]
    chips.sort(key=lambda c: -hops(c))
    codes = [c[0] + 4 * c[1] + 16 * c[2] for c in chips]
    return [sum(codes[4 * w + j] * 64**j for j in range(4)) for w in range(16)]


WORDS = far_first()


def word_at(c):
    word = WORDS[0]
    for w in range(1, 16):
        word = jnp.where(c == w, WORDS[w], word)
    return word


def peers(word, sign):
    x, z, y, core = place()
    found = []
    for j in range(4):
        code = word // 64**j % 64
        px = lax.rem(x + 4 + sign * (code % 4), 4)
        py = lax.rem(y + 4 + sign * (code // 4 % 4), 4)
        pz = lax.rem(z + 4 + sign * (code // 16), 4)
        for pc in (1 - core, core):
            found.append((px * 4 + pz, py * 2 + pc))
    return found


def device(index):
    return {"leaf": index // 8, "sub": lax.rem(index, 8)}


def enter():
    me = my_index()
    barrier = pltpu.get_barrier_semaphore()

    for i in range(1, DEV):
        pl.semaphore_signal(barrier, 1, device_id=device(lax.rem(me + i, DEV)), device_id_type=MESH)


def entered():
    pl.semaphore_wait(pltpu.get_barrier_semaphore(), DEV - 1)


def sent(src, send_sem):
    whole = src.at[pl.ds(0, DEV - 1)]
    pltpu.make_async_copy(whole, whole, send_sem).wait()


def gather_and_send(pick, x, stage, src, dst, send_sem, recv_sem):
    left = iota((1, 128), 1) < VECS
    me = my_index()

    def fill(word):
        for u, (leaf, sub) in enumerate(peers(word, 1)):
            t = leaf * 8 + sub
            for r in range(HALF):
                one = x[pl.ds(pick[t, r], 1), :]
                two = x[pl.ds(pick[t, r + HALF], 1), :]
                stage[u, r : r + 1, :] = jnp.where(left, one, two)
            for r in range(HALF, HALF + 2):
                stage[u, r : r + 1, :] = x[pl.ds(SLOTS + (r - HALF) * DEV + t, 1), :]
        for u, (leaf, sub) in enumerate(peers(word, 1)):
            src[leaf * 8 + sub] = stage[u].astype(BF16)

    def send(word, last=False):
        for u, (leaf, sub) in enumerate(peers(word, 1)):
            t = leaf * 8 + sub
            if last and u == 7:
                pltpu.make_async_copy(src.at[me], dst.at[me], recv_sem.at[me]).start()
                continue
            pltpu.make_async_remote_copy(
                src_ref=src.at[t],
                dst_ref=dst.at[me],
                send_sem=send_sem,
                recv_sem=recv_sem.at[me],
                device_id={"leaf": leaf, "sub": sub},
                device_id_type=MESH,
            ).start()

    fill(WORDS[0])

    def loop(c, carry):
        send(word_at(c))
        fill(word_at(c + 1))
        return carry

    lax.fori_loop(0, 15, loop, 0)
    send(WORDS[15], True)


def receive(arrived, recv_sem, y):
    def some(c, carry):
        ts = [leaf * 8 + sub for leaf, sub in peers(word_at(c), -1)]
        for t in ts:
            pltpu.make_async_copy(arrived.at[t], arrived.at[t], recv_sem.at[t]).wait()
        for t in ts:
            rows = arrived[t].astype(F32)
            at = pl.multiple_of(t * BLOCK, 8)
            y[pl.ds(at, BLOCK), :] = rows
            y[pl.ds(pl.multiple_of(DEV * BLOCK + at, 8), BLOCK), :] = pltpu.roll(rows, 64, 1)
        return carry

    lax.fori_loop(0, 16, some, 0)


def block(k):
    return slice((CROSS - 1 - k) * RANK, (CROSS - k) * RANK)


def above(k):
    return slice(0, (CROSS - 1 - k) * RANK)


def rows_of(j):
    return slice((5 - j) * RANK, (6 - j) * RANK)


def place():
    leaf, sub = lax.axis_index("leaf"), lax.axis_index("sub")
    return leaf // 4, lax.rem(leaf, 4), sub // 2, lax.rem(sub, 2)


def group(phase):
    x, z, y, core = place()
    leaf, sub = lax.axis_index("leaf"), lax.axis_index("sub")
    return [
        (2, core, None),
        (4, y, lambda m, c: {"leaf": leaf, "sub": m * 2 + c}),
        (4, z, lambda m, c: {"leaf": x * 4 + m, "sub": y * 2 + c}),
        (4, x, lambda m, c: {"leaf": m * 4 + z, "sub": y * 2 + c}),
    ][phase]


def share(phase, buf, send_sem, recv_sem, wait=False):
    members, me, target = group(phase)
    leaf, (x, z, y, core) = lax.axis_index("leaf"), place()

    def copy_to(i, c, to):
        return pltpu.make_async_remote_copy(
            src_ref=buf.at[me],
            dst_ref=buf.at[me],
            send_sem=send_sem.at[phase, 2 * i + c],
            recv_sem=recv_sem.at[phase, me],
            device_id=to,
            device_id_type=MESH,
        )

    def act(copy):
        if wait:
            copy.wait_send()
        else:
            copy.start()

    if phase == 0:
        act(copy_to(1, 0, {"leaf": leaf, "sub": y * 2 + 1 - core}))
    else:

        @pl.when(core == 1)
        def _():
            for i in (2, 1, 3):
                for c in range(2):
                    act(copy_to(i, c, target(lax.rem(me + i, members), c)))

    if wait:
        for i in range(1, members):
            other = lax.rem(me + i, members)
            pltpu.make_async_copy(buf.at[other], buf.at[other], recv_sem.at[phase, other]).wait()


def fold(a):
    return jnp.concatenate([a[:32], a[32:]], axis=1)


def unfold(a):
    return jnp.concatenate([a[:, :64], a[:, 64:]], axis=0)


def kernel(
    counts,
    slots_h,
    vec_h,
    inverse_h,
    left_h,
    right_h,
    out_h,
    slots_ref,
    vec,
    out,
    inverse,
    left,
    right,
    pick_v,
    pick,
    rank_ref,
    flat_v,
    flat,
    x,
    stage,
    src1,
    dst1,
    src2,
    dst2,
    y,
    inv_v,
    inv,
    back_v,
    back,
    field,
    v_a,
    v_b,
    v_c,
    v_d,
    g_a,
    g_b,
    g_c,
    g_d,
    partner,
    load_sem,
    index_sem,
    send_sem,
    recv1,
    recv2,
    send_v,
    recv_v,
    send_g,
    recv_g,
):
    scale = [1.0 / math.sqrt(ROWS * 2**k) for k in range(CROSS)]
    with jax.named_scope("enter"):
        loads = [
            pltpu.make_async_copy(h, v, load_sem.at[i])
            for i, (h, v) in enumerate(
                (
                    (slots_h, slots_ref),
                    (vec_h, vec),
                    (left_h, left),
                    (right_h, right),
                    (inverse_h, inverse),
                )
            )
        ]
        for load in loads:
            load.start()
        enter()
    with jax.named_scope("route"):
        loads[0].wait()
        live, owner, ranks, base, total = route(counts, slots_ref, rank_ref)
        flat_v[...] = jnp.clip(jnp.where(live, bucket_row(owner, ranks), 0), 0, 2 * DEV * BLOCK - 1)
        both = total[:, :128].astype(I32)
        source = both * 128 + pltpu.roll(both, 64, 1)
        lane128 = iota((DEV, 128), 1)
        pick_v[...] = jnp.clip(jnp.where(lane128 < PEER, source, 0), 0, SLOTS - 1)
        pick_copy = pltpu.make_async_copy(pick_v, pick, index_sem.at[0])
        pick_copy.start()
        flat_copy = pltpu.make_async_copy(flat_v, flat, index_sem.at[1])
        flat_copy.start()
        position = total[:, 128:]
        x[SLOTS : SLOTS + DEV, :] = jnp.where(lane128.astype(F32) < base, position, 64.0)
        x[SLOTS + DEV :, :] = pltpu.roll(position, 64, 1)
    with jax.named_scope("rows"):
        loads[1].wait()
        for a in range(40):
            part = vec[:, a * 128 : (a + 1) * 128].astype(F32)
            x[a * 128 : (a + 1) * 128, :] = jnp.concatenate([part, part], axis=0).T
        for u in range(8):
            stage[u] = jnp.zeros((BLOCK, 128), F32)
        pick_copy.wait()
    with jax.named_scope("entered"):
        entered()
    with jax.named_scope("send"):
        gather_and_send(pick, x, stage, src1, dst1, send_sem.at[0], recv1)
    with jax.named_scope("gram"):
        loads[2].wait()
        loads[3].wait()
        gram = jnp.zeros((CROSS * RANK - RANK, CROSS * RANK), F32)
        for c in range(4):
            at = slice(c * 1024, (c + 1) * 1024)
            gram = gram + dot_nt(
                left[LOCAL : LOCAL + 6, :, at].reshape(6 * RANK, 1024),
                right[LOCAL:, :, at].reshape(CROSS * RANK, 1024),
            )
        core = group(0)[1]
        g_a[core] = jnp.zeros((192, 256), BF16)
        for j in range(CROSS - 1):
            for k in range(j + 1, CROSS):
                g_a[core, rows_of(j), block(k)] = gram[
                    j * RANK : (j + 1) * RANK, k * RANK : (k + 1) * RANK
                ].astype(BF16)
        share(0, g_a, send_g, recv_g)
    with jax.named_scope("gram_y"):
        share(0, g_a, send_g, recv_g, wait=True)
        ysum = g_a[0].astype(F32) + g_a[1].astype(F32)
        mine = group(1)[1]
        g_b[mine, :160] = ysum[:160, :128].astype(BF16)
        g_b[mine, 160:] = ysum[128:160, 128:].astype(BF16)
    with jax.named_scope("receive"):
        receive(dst1, recv1, y)
    with jax.named_scope("inv"):
        high = y[pl.ds(20, DEV, stride=BLOCK), :]
        low = y[pl.ds(21, DEV, stride=BLOCK), :]
        spot = high.astype(I32) * 64 + low.astype(I32)
        back_v[...] = jnp.clip(jnp.where(lane128 < PEER, spot, 0), 0, ROWS - 1)
        back_copy = pltpu.make_async_copy(back_v, back, index_sem.at[2])
        back_copy.start()
        high_t = high.T
        low_t = low.T
        ids = iota((64, 128), 0).astype(F32)
        lanes = iota((64, 128), 1).astype(F32)
        found = jnp.zeros((64, 128), F32)
        for r in range(PEER):
            hit = jnp.where(ids == high_t[r : r + 1, :], 1.0, 0.0).astype(BF16)
            match = ids == low_t[r : r + 1, :]
            table = jnp.concatenate(
                [jnp.where(match, lanes, 0.0), jnp.where(match, float(r), 0.0)], axis=0
            ).astype(BF16)
            found = found + dot_nt(hit, table)
        whole = found.astype(I32)
        inv_v[...] = jnp.clip(
            jnp.where(iota((64, 128), 1) < 64, bucket_row(whole, pltpu.roll(whole, 64, 1)), 0),
            0,
            2 * DEV * BLOCK - 1,
        )
        inv_copy = pltpu.make_async_copy(inv_v, inv, index_sem.at[3])
        inv_copy.start()
        share(1, g_b, send_g, recv_g)
        inv_copy.wait()
    with jax.named_scope("tree"):

        def some(c, carry):
            for u in range(128):
                x[pl.ds(c * 128 + u, 1), :] = y[pl.ds(inv[c * 2 + u // 64, u % 64], 1), :]
            return carry

        lax.fori_loop(0, ROWS // 128, some, 0)
    with jax.named_scope("leaf"):
        loads[4].wait()
        for l in range(ROWS // LEAF):
            at = slice(l * LEAF, (l + 1) * LEAF)
            field[:, at] = dot_nt(x[at, :].T[:VECS].astype(BF16), inverse[l])
    with jax.named_scope("gram_z"):
        share(1, g_b, send_g, recv_g, wait=True)
        zsum = (g_b[0, :96, :128].astype(F32) + g_b[1, :96, :128].astype(F32)) + (
            g_b[2, :96, :128].astype(F32) + g_b[3, :96, :128].astype(F32)
        )
        g_c[group(2)[1]] = zsum.astype(BF16)
        share(2, g_c, send_g, recv_g)
    with jax.named_scope("local"):
        for level in range(LOCAL):
            size = LEAF * 2**level
            nodes = ROWS // size

            def pair(m, carry):
                at = [pl.multiple_of(m * 2 * size, size), pl.multiple_of(m * 2 * size + size, size)]
                coeff = [
                    (
                        dot_nt(field[:, pl.ds(s, size)].astype(BF16), right[level, :, pl.ds(s, size)])
                        * (1.0 / math.sqrt(size))
                    ).astype(BF16)
                    for s in at
                ]
                for n in range(2):
                    field[:, pl.ds(at[n], size)] -= dot(coeff[1 - n], left[level, :, pl.ds(at[n], size)])
                return carry

            lax.fori_loop(0, nodes // 2, pair, 0, unroll=True)
    with jax.named_scope("gram_x"):
        share(2, g_c, send_g, recv_g, wait=True)
        xsum = (g_c[0, :32].astype(F32) + g_c[1, :32].astype(F32)) + (
            g_c[2, :32].astype(F32) + g_c[3, :32].astype(F32)
        )
        g_d[group(3)[1]] = xsum.astype(BF16)
        share(3, g_d, send_g, recv_g)
    with jax.named_scope("reduce"):
        v = jnp.zeros((VECS, CROSS * RANK), F32)
        for c in range(4):
            at = slice(c * 1024, (c + 1) * 1024)
            v = v + dot_nt(field[:, at].astype(BF16), right[LOCAL:, :, at].reshape(CROSS * RANK, 1024))

    def level_rows(k, g):
        if k == 1:
            return jnp.concatenate([g[128:160], g[160:]], axis=1)[:, above(1)]
        return g[rows_of(k), above(k)]

    def merge(k, va, vb, ga, gb):
        pa = (vb[:, block(k)] * scale[k]).astype(BF16)
        pb = (va[:, block(k)] * scale[k]).astype(BF16)
        if k == CROSS - 1:
            return pa, pb, None
        p2 = jnp.concatenate([pa, pb], axis=1)
        g2 = jnp.concatenate([level_rows(k, ga), level_rows(k, gb)], axis=0).astype(BF16)
        return pa, pb, va[:, above(k)] + vb[:, above(k)] - dot(p2, g2)

    def keep(k, p):
        partner[:, k * RANK : (k + 1) * RANK] = p

    with jax.named_scope("cross_core"):
        core = group(0)[1]
        v_a[core] = jnp.zeros((VECS, 256), F32)
        for k in range(CROSS):
            v_a[core, :, block(k)] = v[:, k * RANK : (k + 1) * RANK]
        share(0, v_a, send_v, recv_v)
        share(0, v_a, send_v, recv_v, wait=True)
        pa, pb, v = merge(0, v_a[0], v_a[1], g_a[0], g_a[1])
        keep(0, jnp.where(core == 0, pa, pb))

    def four(phase, k, v, v_buf, g_buf):
        me = group(phase)[1]
        v = v.astype(BF16).astype(F32)
        if phase == 1:
            v_buf[me, :64] = v[:, :128].astype(BF16)
            v_buf[me, 64:] = fold(v[:, 128:]).astype(BF16)
        elif phase == 2:
            v_buf[me] = v.astype(BF16)
        else:
            v_buf[me] = fold(v).astype(BF16)
        share(phase, v_buf, send_v, recv_v)
        share(phase, v_buf, send_v, recv_v, wait=True)
        vs = [v_buf[i].astype(F32) for i in range(4)]
        if phase == 1:
            vs = [jnp.concatenate([u[:64], unfold(u[64:])], axis=1) for u in vs]
        elif phase == 3:
            vs = [unfold(u) for u in vs]
        gs = [g_buf[i].astype(F32) for i in range(4)]
        p0, p1, v01 = merge(k, vs[0], vs[1], gs[0], gs[1])
        p2, p3, v23 = merge(k, vs[2], vs[3], gs[2], gs[3])
        keep(k, jnp.where(me < 2, jnp.where(me == 0, p0, p1), jnp.where(me == 2, p2, p3)))
        pa, pb, v = merge(k + 1, v01, v23, gs[0] + gs[1], gs[2] + gs[3])
        keep(k + 1, jnp.where(me < 2, pa, pb))
        return v

    with jax.named_scope("cross_y"):
        v = four(1, 1, v, v_b, g_b)
    with jax.named_scope("cross_z"):
        v = four(2, 3, v, v_c, g_c)
    with jax.named_scope("cross_x"):
        share(3, g_d, send_g, recv_g, wait=True)
        four(3, 5, v, v_d, g_d)
    with jax.named_scope("finish"):
        for c in range(16):
            at = slice(c * LEAF, (c + 1) * LEAF)
            done = field[:, at] - dot(
                partner[:, : CROSS * RANK], left[LOCAL:, :, at].reshape(CROSS * RANK, LEAF)
            )
            x[at, :] = jnp.concatenate([done, done], axis=0).T
        back_copy.wait()
        sent(src1, send_sem.at[0])
    with jax.named_scope("send_back"):
        gather_and_send(back, x, stage, src2, dst2, send_sem.at[1], recv2)
    with jax.named_scope("receive_back"):
        flat_copy.wait()
        receive(dst2, recv2, y)
    with jax.named_scope("output"):
        alive = jnp.where(live_slots(counts, slots_ref[...]), 1, 0)

        def pull(c):
            for u in range(128):
                x[pl.ds(pl.multiple_of(c * 128, 128) + u, 1), :] = y[pl.ds(flat[c, u], 1), :]

        def push(a):
            at = pl.multiple_of(a * 128, 128)
            part = x[pl.ds(at, 128), :].T[:VECS]
            out[:, pl.ds(at, 128)] = jnp.where(slots_ref[pl.ds(a, 1), :] > 0, part, 0.0).astype(BF16)

        slots_ref[...] = alive
        pull(0)

        def step(c, carry):
            pull(c + 1)
            push(c)
            return carry

        lax.fori_loop(0, 39, step, 0)
        push(39)
        store = pltpu.make_async_copy(out, out_h, load_sem.at[0])
        store.start()
        store.wait()
        sent(src2, send_sem.at[1])


def body(vectors, row_counts, tree_slot, leaf_inverse, left_basis, right_basis):
    anywhere = pl.BlockSpec(memory_space=pl.ANY)
    dma = pltpu.SemaphoreType.DMA
    blocks = pltpu.VMEM((DEV, BLOCK, 128), BF16)
    return pl.pallas_call(
        kernel,
        out_shape=jax.ShapeDtypeStruct((VECS, SLOTS), BF16),
        in_specs=[SMEM] + [anywhere] * 5,
        out_specs=anywhere,
        scratch_shapes=[
            pltpu.VMEM((40, 128), I32),
            pltpu.VMEM((VECS, SLOTS), BF16),
            pltpu.VMEM((VECS, SLOTS), BF16),
            pltpu.VMEM(leaf_inverse.shape, BF16),
            pltpu.VMEM(left_basis.shape, BF16),
            pltpu.VMEM(right_basis.shape, BF16),
            pltpu.VMEM((DEV, 128), I32),
            pltpu.SMEM((DEV, 128), I32),
            pltpu.VMEM((40, 128), F32),
            pltpu.VMEM((40, 128), I32),
            pltpu.SMEM((40, 128), I32),
            pltpu.VMEM((SLOTS + 2 * DEV, 128), F32),
            pltpu.VMEM((8, BLOCK, 128), F32),
            blocks,
            blocks,
            blocks,
            blocks,
            pltpu.VMEM((2 * DEV * BLOCK, 128), F32),
            pltpu.VMEM((64, 128), I32),
            pltpu.SMEM((64, 128), I32),
            pltpu.VMEM((DEV, 128), I32),
            pltpu.SMEM((DEV, 128), I32),
            pltpu.VMEM((VECS, ROWS), F32),
            pltpu.VMEM((2, VECS, 256), F32),
            pltpu.VMEM((4, 96, 128), BF16),
            pltpu.VMEM((4, VECS, 128), BF16),
            pltpu.VMEM((4, 32, 128), BF16),
            pltpu.VMEM((2, 192, 256), BF16),
            pltpu.VMEM((4, 192, 128), BF16),
            pltpu.VMEM((4, 96, 128), BF16),
            pltpu.VMEM((4, 32, 128), BF16),
            pltpu.VMEM((VECS, 256), BF16),
            dma((5,)),
            dma((4,)),
            dma((2,)),
            dma((DEV,)),
            dma((DEV,)),
            dma((4, 8)),
            dma((4, 4)),
            dma((4, 8)),
            dma((4, 4)),
        ],
        compiler_params=pltpu.CompilerParams(collective_id=0, has_side_effects=True),
        name="apply",
    )(row_counts, tree_slot.reshape(40, 128), vectors, leaf_inverse, left_basis, right_basis)


def solution(mesh):
    both = ("leaf", "sub")
    return jax.shard_map(
        body,
        mesh=mesh,
        in_specs=(
            P(None, both),
            P(),
            P(both),
            P(both, None, None),
            P(None, None, both),
            P(None, None, both),
        ),
        out_specs=P(None, both),
        check_vma=False,
    )
```

```python
import functools
import math

import jax
import jax.numpy as jnp
import numpy as np
from jax import lax
from jax.experimental import pallas as pl
from jax.experimental.pallas import tpu as pltpu
from jax.sharding import PartitionSpec as P

DEV = 128
PEER = 40
HALF = 20
BLOCK = 20
ROWS = 4096
SLOTS = 5120
VECS = 64
LEAF = 256
RANK = 32
LOCAL = 4
CROSS = 7
F32 = jnp.float32
BF16 = jnp.bfloat16
I32 = jnp.int32
VMEM = pl.BlockSpec(memory_space=pltpu.VMEM)
SMEM = pl.BlockSpec(memory_space=pltpu.SMEM)
NT = (((1,), (1,)), ((), ()))
MESH = pl.DeviceIdType.MESH


FAR = (2, 1, 3, 0)
PAIRS = sorted(((dx, dz) for dx in FAR for dz in FAR), key=lambda c: -sum(min(d, 4 - d) for d in c))
ORDER = [(dx, dy, dz, dc) for dx, dz in PAIRS for dy in FAR for dc in (1, 0)]
CODES = np.array([32 * dx + 8 * dz + 2 * dy + dc for dx, dy, dz, dc in ORDER], np.int32).reshape(16, 8).T.reshape(-1)


def place():
    leaf, sub = lax.axis_index("leaf"), lax.axis_index("sub")
    return leaf // 4, lax.rem(leaf, 4), sub // 2, lax.rem(sub, 2)


def wrapped(at, d):
    return lax.rem(at + 4 + d, 4)


def chosen(n, values):
    value = values[0]
    for k in range(1, len(values)):
        value = jnp.where(n == k, values[k], value)
    return value


def group_of(c, sign):
    x, z, y, core = place()
    if isinstance(c, int):
        dx, dz = PAIRS[c]
    else:
        dx, dz = chosen(c, [p[0] for p in PAIRS]), chosen(c, [p[1] for p in PAIRS])
    leaf = wrapped(x, sign * dx) * 4 + wrapped(z, sign * dz)
    return [{"leaf": leaf, "sub": wrapped(y, sign * dy) * 2 + pc} for dy in FAR for pc in (1 - core, core)]


def iota(shape, dim):
    return lax.broadcasted_iota(I32, shape, dim)


def dot_nt(a, b):
    return lax.dot_general(a, b, NT, preferred_element_type=F32)


def dot(a, b):
    return jnp.dot(a, b, preferred_element_type=F32)


def bucket_row(label, rank):
    owner = (label & 15) * 8 + (label >> 4)
    return jnp.where(rank < HALF, owner * BLOCK + rank, DEV * BLOCK + owner * BLOCK + rank - HALF)


def live_slots(counts, slots):
    index = iota((40, 128), 0) * 128 + iota((40, 128), 1)
    mine = lax.axis_index("leaf") * 8 + lax.axis_index("sub")
    return (index < counts[mine]) & (slots >= 0)


def route(counts, slots_ref, codes, rank_ref):
    slots = slots_ref[...]
    live = live_slots(counts, slots)
    x, z, y, core = place()
    away = (
        (((slots >> 17) + 4 - x) & 3) * 32
        + (((slots >> 15) + 4 - z) & 3) * 8
        + (((slots >> 13) + 4 - y) & 3) * 2
        + (((slots >> 12) + 2 - core) & 1)
    )
    owner = jnp.where(live, away, DEV)
    high = ((slots & 4095) >> 6).astype(F32)
    low = (slots & 63).astype(F32)
    ids = codes[...]
    before = jnp.where(iota((128, 256), 0) < iota((128, 256), 1), 1.0, 0.0).astype(BF16)
    start = (iota((DEV, 128), 0) * 64).astype(F32)
    base = start
    for a in range(40):
        hit = ids == owner[a : a + 1, :]
        earlier = dot(jnp.where(hit, 1.0, 0.0).astype(BF16), before)
        rank_ref[a : a + 1, :] = jnp.sum(jnp.where(hit, base + earlier[:, :128], 0.0), axis=0, keepdims=True)
        base = base + earlier[:, 128:]
    found = rank_ref[...].astype(I32)
    ranks = found & 63
    r64 = iota((64, 128), 0)
    lane = iota((64, 128), 1).astype(F32)
    total = jnp.zeros((DEV, 256), F32)
    for a in range(40):
        hit = jnp.where(ids == owner[a : a + 1, :], 1.0, 0.0).astype(BF16)
        match = r64 == ranks[a : a + 1, :]
        table = jnp.concatenate(
            [
                jnp.where(match, float(a), 0.0),
                jnp.where(match, lane, 0.0),
                jnp.where(match, high[a : a + 1, :], 0.0),
                jnp.where(match, low[a : a + 1, :], 0.0),
            ],
            axis=0,
        ).astype(BF16)
        total = total + dot_nt(hit, table)
    return live, found >> 6, ranks, base - start, total


def enter():
    barrier = pltpu.get_barrier_semaphore()
    for c in range(16):
        for to in group_of(c, 1)[: 8 if c < 15 else 7]:
            pl.semaphore_signal(barrier, 1, device_id=to, device_id_type=MESH)


def entered():
    pl.semaphore_wait(pltpu.get_barrier_semaphore(), DEV - 1)


def await_bytes(part, sem):
    pltpu.make_async_copy(part, part, sem).wait()


def sent(src, send_sem):
    await_bytes(src.at[pl.ds(0, 5 * (DEV - 1))], send_sem)


def remote(src, dst, send_sem, recv_sem, to):
    return pltpu.make_async_remote_copy(
        src_ref=src, dst_ref=dst, send_sem=send_sem, recv_sem=recv_sem, device_id=to, device_id_type=MESH
    )


def gather_and_send(pick, x, stage, src, dst, send_sem, recv_sem, sign):
    left = iota((1, 128), 1) < VECS

    def fill(c):
        for u in range(8):
            for r in range(HALF):
                one = x[pl.ds(pick.at[r, pl.ds(16 * u, 16)][c], 1), :]
                two = x[pl.ds(pick.at[r + HALF, pl.ds(16 * u, 16)][c], 1), :]
                stage[u, r : r + 1, :] = jnp.where(left, one, two)
            for q in range(5):
                src[(c * 8 + u) * 5 + q] = stage[u, 4 * q : 4 * q + 4, :].astype(BF16)

    def send(c):
        for u, to in enumerate(group_of(c, sign)):
            i = c * 8 + u
            part = pl.ds(i * 5, 5)
            if isinstance(c, int) and i == DEV - 1:
                pltpu.make_async_copy(src.at[part], dst.at[part], recv_sem.at[c]).start()
            else:
                remote(src.at[part], dst.at[part], send_sem, recv_sem.at[c], to).start()

    fill(0)

    def loop(c, carry):
        send(c)
        fill(c + 1)
        return carry

    lax.fori_loop(0, 15, loop, 0)
    send(15)


def receive(arrived, recv_sem, y):
    for j in range(16):
        await_bytes(arrived.at[pl.ds(40 * j, 40)], recv_sem.at[j])
        for i in range(8 * j, 8 * j + 8):
            for q in range(5):
                rows = arrived[5 * i + q].astype(F32)
                at = i * BLOCK + 4 * q
                y[at : at + 4, :] = rows
                y[DEV * BLOCK + at : DEV * BLOCK + at + 4, :] = pltpu.roll(rows, 64, 1)


def block(k):
    return slice((CROSS - 1 - k) * RANK, (CROSS - k) * RANK)


def above(k):
    return slice(0, (CROSS - 1 - k) * RANK)


def rows_of(j):
    return slice((5 - j) * RANK, (6 - j) * RANK)


def place():
    leaf, sub = lax.axis_index("leaf"), lax.axis_index("sub")
    return leaf // 4, lax.rem(leaf, 4), sub // 2, lax.rem(sub, 2)


def group(phase):
    x, z, y, core = place()
    leaf, sub = lax.axis_index("leaf"), lax.axis_index("sub")
    return [
        (2, core, None),
        (4, y, lambda m, c: {"leaf": leaf, "sub": m * 2 + c}),
        (4, z, lambda m, c: {"leaf": x * 4 + m, "sub": y * 2 + c}),
        (4, x, lambda m, c: {"leaf": m * 4 + z, "sub": y * 2 + c}),
    ][phase]


def share(phase, buf, send_sem, recv_sem, wait=False):
    members, me, target = group(phase)
    leaf, (x, z, y, core) = lax.axis_index("leaf"), place()
    others = buf.at[pl.ds(0, members - 1)]

    def copy_to(c, to):
        return remote(buf.at[me], buf.at[me], send_sem.at[phase, c], recv_sem.at[phase], to)

    if phase == 0:
        if not wait:
            copy_to(0, {"leaf": leaf, "sub": y * 2 + 1 - core}).start()
        else:
            await_bytes(others, send_sem.at[phase, 0])
    else:

        @pl.when(core == 1)
        def _():
            for c in range(2):
                if wait:
                    await_bytes(others, send_sem.at[phase, c])
                    continue
                for i in (2, 1, 3):
                    copy_to(c, target(lax.rem(me + i, members), c)).start()

    if wait:
        await_bytes(others, recv_sem.at[phase])


def fold(a):
    return jnp.concatenate([a[:32], a[32:]], axis=1)


def unfold(a):
    return jnp.concatenate([a[:, :64], a[:, 64:]], axis=0)


def kernel(
    counts,
    codes_h,
    slots_h,
    vec_h,
    inverse_h,
    left_h,
    right_h,
    out_h,
    codes,
    slots_ref,
    vec,
    out,
    inverse,
    left,
    right,
    pick_v,
    pick,
    rank_ref,
    flat_v,
    flat,
    x,
    stage,
    pos_src,
    pos_dst,
    src1,
    dst1,
    src2,
    dst2,
    y,
    inv_v,
    inv,
    back_v,
    back,
    field,
    v_a,
    v_b,
    v_c,
    v_d,
    g_a,
    g_b,
    g_c,
    g_d,
    partner,
    load_sem,
    pos_sem,
    index_sem,
    send_sem,
    recv1,
    recv2,
    send_v,
    recv_v,
    send_g,
    recv_g,
):
    scale = [1.0 / math.sqrt(ROWS * 2**k) for k in range(CROSS)]
    with jax.named_scope("enter"):
        loads = [
            pltpu.make_async_copy(h, v, load_sem.at[i])
            for i, (h, v) in enumerate(
                (
                    (codes_h, codes),
                    (slots_h, slots_ref),
                    (vec_h, vec),
                    (left_h, left),
                    (right_h, right),
                    (inverse_h, inverse),
                )
            )
        ]
        for load in loads:
            load.start()
        enter()
    with jax.named_scope("route"):
        loads[0].wait()
        loads[1].wait()
        live, owner, ranks, base, total = route(counts, slots_ref, codes, rank_ref)
        rows = jnp.where(live, bucket_row(owner, ranks), 0).astype(F32)
        rows = jnp.concatenate([rows, jnp.zeros((DEV - 40, 128), F32)], axis=0).T.astype(I32)
        flat_v[...] = jnp.clip(rows, 0, 2 * DEV * BLOCK - 1)
        both = total[:, :128].astype(I32)
        source = both * 128 + pltpu.roll(both, 64, 1)
        lane128 = iota((DEV, 128), 1)
        pick_v[...] = jnp.clip(source.astype(F32).T[:PEER].astype(I32), 0, SLOTS - 1)
        pick_copy = pltpu.make_async_copy(pick_v, pick, index_sem.at[0])
        pick_copy.start()
        flat_copy = pltpu.make_async_copy(flat_v, flat, index_sem.at[1])
        flat_copy.start()
        position = total[:, 128:]
        spot = position * 64.0 + pltpu.roll(position, 64, 1)
        pos_src[...] = jnp.where(lane128.astype(F32) < base, spot, float(ROWS)).reshape(DEV, 1, 128)
        pos_dst[DEV - 1] = pos_src[DEV - 1]
    with jax.named_scope("rows"):
        loads[2].wait()
        for a in range(40):
            part = vec[:, a * 128 : (a + 1) * 128].astype(F32)
            x[a * 128 : (a + 1) * 128, :] = jnp.concatenate([part, part], axis=0).T
        pick_copy.wait()
    with jax.named_scope("entered"):
        entered()
    with jax.named_scope("positions"):
        for c in range(16):
            for u, to in enumerate(group_of(c, 1)[: 8 if c < 15 else 7]):
                i = 16 * u + c
                remote(pos_src.at[i], pos_dst.at[i], pos_sem.at[0], pos_sem.at[1], to).start()
    with jax.named_scope("send"):
        gather_and_send(pick, x, stage, src1, dst1, send_sem.at[0], recv1, 1)
    with jax.named_scope("gram"):
        loads[3].wait()
        loads[4].wait()
        gram = jnp.zeros((CROSS * RANK - RANK, CROSS * RANK), F32)
        for c in range(4):
            at = slice(c * 1024, (c + 1) * 1024)
            gram = gram + dot_nt(
                left[LOCAL : LOCAL + 6, :, at].reshape(6 * RANK, 1024),
                right[LOCAL:, :, at].reshape(CROSS * RANK, 1024),
            )
        core = group(0)[1]
        g_a[core] = jnp.zeros((192, 256), BF16)
        for j in range(CROSS - 1):
            for k in range(j + 1, CROSS):
                g_a[core, rows_of(j), block(k)] = gram[
                    j * RANK : (j + 1) * RANK, k * RANK : (k + 1) * RANK
                ].astype(BF16)
        share(0, g_a, send_g, recv_g)
    with jax.named_scope("inv"):
        await_bytes(pos_dst.at[pl.ds(0, DEV - 1)], pos_sem.at[1])
        await_bytes(pos_src.at[pl.ds(0, DEV - 1)], pos_sem.at[0])
        spot = pos_dst[...].reshape(DEV, 128).astype(I32)
        back_v[...] = jnp.clip(spot.astype(F32).T[:PEER].astype(I32), 0, ROWS - 1)
        back_copy = pltpu.make_async_copy(back_v, back, index_sem.at[2])
        back_copy.start()
        high_t = (spot >> 6).astype(F32).T
        low_t = (spot & 63).astype(F32).T
        ids = iota((64, 128), 0).astype(F32)
        lanes = iota((64, 128), 1).astype(F32)
        found = jnp.zeros((64, 128), F32)
        for r in range(PEER):
            hit = jnp.where(ids == high_t[r : r + 1, :], 1.0, 0.0).astype(BF16)
            match = ids == low_t[r : r + 1, :]
            table = jnp.concatenate(
                [jnp.where(match, lanes, 0.0), jnp.where(match, float(r), 0.0)], axis=0
            ).astype(BF16)
            found = found + dot_nt(hit, table)
        whole = found.astype(I32)
        inv_v[...] = jnp.clip(
            jnp.where(iota((64, 128), 1) < 64, bucket_row(whole, pltpu.roll(whole, 64, 1)), 0),
            0,
            2 * DEV * BLOCK - 1,
        )
        inv_copy = pltpu.make_async_copy(inv_v, inv, index_sem.at[3])
        inv_copy.start()
    with jax.named_scope("gram_y"):
        share(0, g_a, send_g, recv_g, wait=True)
        ysum = g_a[0].astype(F32) + g_a[1].astype(F32)
        mine = group(1)[1]
        g_b[mine, :160] = ysum[:160, :128].astype(BF16)
        g_b[mine, 160:] = ysum[128:160, 128:].astype(BF16)
    with jax.named_scope("receive"):
        receive(dst1, recv1, y)
        share(1, g_b, send_g, recv_g)
        inv_copy.wait()
    with jax.named_scope("tree"):
        loads[5].wait()

        def pull(c, carry):
            for u in range(128):
                at = pl.ds(u * 32 + c, 1)
                x[at, :] = y[pl.ds(inv.at[u // 2, pl.ds(u % 2 * 32, 32)][c], 1), :]
            return carry

        lax.fori_loop(0, 32, pull, 0)
    with jax.named_scope("leaf"):
        for l in range(ROWS // LEAF):
            at = slice(l * LEAF, (l + 1) * LEAF)
            field[:, at] = dot_nt(x[at, :].T[:VECS].astype(BF16), inverse[l])
    with jax.named_scope("gram_z"):
        share(1, g_b, send_g, recv_g, wait=True)
        zsum = (g_b[0, :96, :128].astype(F32) + g_b[1, :96, :128].astype(F32)) + (
            g_b[2, :96, :128].astype(F32) + g_b[3, :96, :128].astype(F32)
        )
        g_c[group(2)[1]] = zsum.astype(BF16)
        share(2, g_c, send_g, recv_g)
    with jax.named_scope("local"):
        for level in range(LOCAL):
            size = LEAF * 2**level
            nodes = ROWS // size

            def pair(m, carry):
                at = [pl.multiple_of(m * 2 * size, size), pl.multiple_of(m * 2 * size + size, size)]
                coeff = [
                    (
                        dot_nt(field[:, pl.ds(s, size)].astype(BF16), right[level, :, pl.ds(s, size)])
                        * (1.0 / math.sqrt(size))
                    ).astype(BF16)
                    for s in at
                ]
                for n in range(2):
                    field[:, pl.ds(at[n], size)] -= dot(coeff[1 - n], left[level, :, pl.ds(at[n], size)])
                return carry

            lax.fori_loop(0, nodes // 2, pair, 0, unroll=True)
    with jax.named_scope("gram_x"):
        share(2, g_c, send_g, recv_g, wait=True)
        xsum = (g_c[0, :32].astype(F32) + g_c[1, :32].astype(F32)) + (
            g_c[2, :32].astype(F32) + g_c[3, :32].astype(F32)
        )
        g_d[group(3)[1]] = xsum.astype(BF16)
        share(3, g_d, send_g, recv_g)
    with jax.named_scope("reduce"):
        v = jnp.zeros((VECS, CROSS * RANK), F32)
        for c in range(4):
            at = slice(c * 1024, (c + 1) * 1024)
            v = v + dot_nt(field[:, at].astype(BF16), right[LOCAL:, :, at].reshape(CROSS * RANK, 1024))

    def level_rows(k, g):
        if k == 1:
            return jnp.concatenate([g[128:160], g[160:]], axis=1)[:, above(1)]
        return g[rows_of(k), above(k)]

    def merge(k, va, vb, ga, gb):
        pa = (vb[:, block(k)] * scale[k]).astype(BF16)
        pb = (va[:, block(k)] * scale[k]).astype(BF16)
        if k == CROSS - 1:
            return pa, pb, None
        p2 = jnp.concatenate([pa, pb], axis=1)
        g2 = jnp.concatenate([level_rows(k, ga), level_rows(k, gb)], axis=0).astype(BF16)
        return pa, pb, va[:, above(k)] + vb[:, above(k)] - dot(p2, g2)

    def keep(k, p):
        partner[:, k * RANK : (k + 1) * RANK] = p

    with jax.named_scope("cross_core"):
        core = group(0)[1]
        v_a[core] = jnp.zeros((VECS, 256), F32)
        for k in range(CROSS):
            v_a[core, :, block(k)] = v[:, k * RANK : (k + 1) * RANK]
        share(0, v_a, send_v, recv_v)
        share(0, v_a, send_v, recv_v, wait=True)
        pa, pb, v = merge(0, v_a[0], v_a[1], g_a[0], g_a[1])
        keep(0, jnp.where(core == 0, pa, pb))

    def four(phase, k, v, v_buf, g_buf):
        me = group(phase)[1]
        v = v.astype(BF16).astype(F32)
        if phase == 1:
            v_buf[me, :64] = v[:, :128].astype(BF16)
            v_buf[me, 64:] = fold(v[:, 128:]).astype(BF16)
        elif phase == 2:
            v_buf[me] = v.astype(BF16)
        else:
            v_buf[me] = fold(v).astype(BF16)
        share(phase, v_buf, send_v, recv_v)
        share(phase, v_buf, send_v, recv_v, wait=True)
        vs = [v_buf[i].astype(F32) for i in range(4)]
        if phase == 1:
            vs = [jnp.concatenate([u[:64], unfold(u[64:])], axis=1) for u in vs]
        elif phase == 3:
            vs = [unfold(u) for u in vs]
        gs = [g_buf[i].astype(F32) for i in range(4)]
        p0, p1, v01 = merge(k, vs[0], vs[1], gs[0], gs[1])
        p2, p3, v23 = merge(k, vs[2], vs[3], gs[2], gs[3])
        keep(k, jnp.where(me < 2, jnp.where(me == 0, p0, p1), jnp.where(me == 2, p2, p3)))
        pa, pb, v = merge(k + 1, v01, v23, gs[0] + gs[1], gs[2] + gs[3])
        keep(k + 1, jnp.where(me < 2, pa, pb))
        return v

    with jax.named_scope("cross_y"):
        v = four(1, 1, v, v_b, g_b)
    with jax.named_scope("cross_z"):
        v = four(2, 3, v, v_c, g_c)
    with jax.named_scope("cross_x"):
        share(3, g_d, send_g, recv_g, wait=True)
        four(3, 5, v, v_d, g_d)
    with jax.named_scope("finish"):
        for c in range(16):
            at = slice(c * LEAF, (c + 1) * LEAF)
            done = field[:, at] - dot(
                partner[:, : CROSS * RANK], left[LOCAL:, :, at].reshape(CROSS * RANK, LEAF)
            )
            x[at, :] = jnp.concatenate([done, done], axis=0).T
        back_copy.wait()
        sent(src1, send_sem.at[0])
    with jax.named_scope("send_back"):
        gather_and_send(back, x, stage, src2, dst2, send_sem.at[1], recv2, -1)
    with jax.named_scope("receive_back"):
        flat_copy.wait()
        receive(dst2, recv2, y)
    with jax.named_scope("output"):
        alive = jnp.where(live_slots(counts, slots_ref[...]), 1, 0)

        slots_ref[...] = alive

        def pull_slots(a):
            for u in range(128):
                x[pl.ds(pl.multiple_of(a * 128, 128) + u, 1), :] = y[pl.ds(flat.at[u][a], 1), :]

        def push(a):
            at = pl.multiple_of(a * 128, 128)
            part = x[pl.ds(at, 128), :].T[:VECS]
            out[:, pl.ds(at, 128)] = jnp.where(slots_ref[pl.ds(a, 1), :] > 0, part, 0.0).astype(BF16)

        pull_slots(0)

        def next_slots(a, carry):
            push(a)
            pull_slots(a + 1)
            return carry

        lax.fori_loop(0, 39, next_slots, 0)
        push(39)
        store = pltpu.make_async_copy(out, out_h, load_sem.at[0])
        store.start()
        store.wait()
        sent(src2, send_sem.at[1])


def body(vectors, row_counts, tree_slot, leaf_inverse, left_basis, right_basis):
    anywhere = pl.BlockSpec(memory_space=pl.ANY)
    dma = pltpu.SemaphoreType.DMA
    blocks = pltpu.VMEM((DEV * 5, 4, 128), BF16)
    return pl.pallas_call(
        kernel,
        out_shape=jax.ShapeDtypeStruct((VECS, SLOTS), BF16),
        in_specs=[SMEM] + [anywhere] * 6,
        out_specs=anywhere,
        scratch_shapes=[
            pltpu.VMEM((DEV, 128), I32),
            pltpu.VMEM((40, 128), I32),
            pltpu.VMEM((VECS, SLOTS), BF16),
            pltpu.VMEM((VECS, SLOTS), BF16),
            pltpu.VMEM(leaf_inverse.shape, BF16),
            pltpu.VMEM(left_basis.shape, BF16),
            pltpu.VMEM(right_basis.shape, BF16),
            pltpu.VMEM((PEER, DEV), I32),
            pltpu.SMEM((PEER, DEV), I32),
            pltpu.VMEM((40, 128), F32),
            pltpu.VMEM((DEV, 128), I32),
            pltpu.SMEM((DEV, 128), I32),
            pltpu.VMEM((SLOTS, 128), F32),
            pltpu.VMEM((8, BLOCK, 128), F32),
            pltpu.VMEM((DEV, 1, 128), F32),
            pltpu.VMEM((DEV, 1, 128), F32),
            blocks,
            blocks,
            blocks,
            blocks,
            pltpu.VMEM((2 * DEV * BLOCK, 128), F32),
            pltpu.VMEM((64, 128), I32),
            pltpu.SMEM((64, 128), I32),
            pltpu.VMEM((PEER, DEV), I32),
            pltpu.SMEM((PEER, DEV), I32),
            pltpu.VMEM((VECS, ROWS), F32),
            pltpu.VMEM((2, VECS, 256), F32),
            pltpu.VMEM((4, 96, 128), BF16),
            pltpu.VMEM((4, VECS, 128), BF16),
            pltpu.VMEM((4, 32, 128), BF16),
            pltpu.VMEM((2, 192, 256), BF16),
            pltpu.VMEM((4, 192, 128), BF16),
            pltpu.VMEM((4, 96, 128), BF16),
            pltpu.VMEM((4, 32, 128), BF16),
            pltpu.VMEM((VECS, 256), BF16),
            dma((6,)),
            dma((2,)),
            dma((4,)),
            dma((2,)),
            dma((16,)),
            dma((16,)),
            dma((4, 2)),
            dma((4,)),
            dma((4, 2)),
            dma((4,)),
        ],
        compiler_params=pltpu.CompilerParams(collective_id=0, has_side_effects=True),
        name="apply",
    )(
        row_counts,
        jnp.asarray(np.repeat(CODES[:, None], 128, 1)),
        tree_slot.reshape(40, 128), vectors, leaf_inverse, left_basis, right_basis)


def solution(mesh):
    both = ("leaf", "sub")
    return jax.shard_map(
        body,
        mesh=mesh,
        in_specs=(
            P(None, both),
            P(),
            P(both),
            P(both, None, None),
            P(None, None, both),
            P(None, None, both),
        ),
        out_specs=P(None, both),
        check_vma=False,
    )
```

```python
import functools
import math

import jax
import jax.numpy as jnp
import numpy as np
from jax import lax
from jax.experimental import pallas as pl
from jax.experimental.pallas import tpu as pltpu
from jax.sharding import PartitionSpec as P

DEV = 128
PEER = 40
HALF = 20
BLOCK = 20
ROWS = 4096
SLOTS = 5120
VECS = 64
LEAF = 256
RANK = 32
LOCAL = 4
CROSS = 7
LEVELS = 11
F32 = jnp.float32
BF16 = jnp.bfloat16
I32 = jnp.int32
VMEM = pl.BlockSpec(memory_space=pltpu.VMEM)
SMEM = pl.BlockSpec(memory_space=pltpu.SMEM)
NT = (((1,), (1,)), ((), ()))
MESH = pl.DeviceIdType.MESH


FAR = (2, 1, 3, 0)
PAIRS = sorted(((dx, dz) for dx in FAR for dz in FAR), key=lambda c: -sum(min(d, 4 - d) for d in c))
ORDER = [(dx, dy, dz, dc) for dx, dz in PAIRS for dy in FAR for dc in (1, 0)]
CODES = np.array([32 * dx + 8 * dz + 2 * dy + dc for dx, dy, dz, dc in ORDER], np.int32).reshape(16, 8).T.reshape(-1)


def place():
    leaf, sub = lax.axis_index("leaf"), lax.axis_index("sub")
    return leaf // 4, lax.rem(leaf, 4), sub // 2, lax.rem(sub, 2)


def wrapped(at, d):
    return lax.rem(at + 4 + d, 4)


def chosen(n, values):
    value = values[0]
    for k in range(1, len(values)):
        value = jnp.where(n == k, values[k], value)
    return value


def group_of(c, sign):
    x, z, y, core = place()
    if isinstance(c, int):
        dx, dz = PAIRS[c]
    else:
        dx, dz = chosen(c, [p[0] for p in PAIRS]), chosen(c, [p[1] for p in PAIRS])
    leaf = wrapped(x, sign * dx) * 4 + wrapped(z, sign * dz)
    return [{"leaf": leaf, "sub": wrapped(y, sign * dy) * 2 + pc} for dy in FAR for pc in (1 - core, core)]


def iota(shape, dim):
    return lax.broadcasted_iota(I32, shape, dim)


def dot_nt(a, b):
    return lax.dot_general(a, b, NT, preferred_element_type=F32)


def dot(a, b):
    return jnp.dot(a, b, preferred_element_type=F32)


def bucket_row(label, rank):
    owner = (label & 15) * 8 + (label >> 4)
    return jnp.where(rank < HALF, owner * BLOCK + rank, DEV * BLOCK + owner * BLOCK + rank - HALF)


def live_slots(counts, slots):
    index = iota((40, 128), 0) * 128 + iota((40, 128), 1)
    mine = lax.axis_index("leaf") * 8 + lax.axis_index("sub")
    return (index < counts[mine]) & (slots >= 0)


def route(counts, slots_ref, codes, rank_ref):
    slots = slots_ref[...]
    live = live_slots(counts, slots)
    x, z, y, core = place()
    away = (
        (((slots >> 17) + 4 - x) & 3) * 32
        + (((slots >> 15) + 4 - z) & 3) * 8
        + (((slots >> 13) + 4 - y) & 3) * 2
        + (((slots >> 12) + 2 - core) & 1)
    )
    owner = jnp.where(live, away, DEV)
    high = ((slots & 4095) >> 6).astype(F32)
    low = (slots & 63).astype(F32)
    ids = codes[...]
    before = jnp.where(iota((128, 256), 0) < iota((128, 256), 1), 1.0, 0.0).astype(BF16)
    start = (iota((DEV, 128), 0) * 64).astype(F32)
    base = start
    for a in range(40):
        hit = ids == owner[a : a + 1, :]
        earlier = dot(jnp.where(hit, 1.0, 0.0).astype(BF16), before)
        rank_ref[a : a + 1, :] = jnp.sum(jnp.where(hit, base + earlier[:, :128], 0.0), axis=0, keepdims=True)
        base = base + earlier[:, 128:]
    found = rank_ref[...].astype(I32)
    ranks = found & 63
    r64 = iota((64, 128), 0)
    lane = iota((64, 128), 1).astype(F32)
    total = jnp.zeros((DEV, 256), F32)
    def tables(a):
        hit = jnp.where(ids == owner[a : a + 1, :], 1.0, 0.0).astype(BF16)
        match = r64 == ranks[a : a + 1, :]
        table = jnp.concatenate(
            [
                jnp.where(match, float(a), 0.0),
                jnp.where(match, lane, 0.0),
                jnp.where(match, high[a : a + 1, :], 0.0),
                jnp.where(match, low[a : a + 1, :], 0.0),
            ],
            axis=0,
        ).astype(BF16)
        return hit, table

    for a in range(0, 40, 2):
        hits, parts = zip(tables(a), tables(a + 1))
        total = total + dot_nt(jnp.concatenate(hits, axis=1), jnp.concatenate(parts, axis=1))
    return live, found >> 6, ranks, base - start, total


def enter():
    barrier = pltpu.get_barrier_semaphore()
    for c in range(16):
        for to in group_of(c, 1)[: 8 if c < 15 else 7]:
            pl.semaphore_signal(barrier, 1, device_id=to, device_id_type=MESH)


def entered():
    pl.semaphore_wait(pltpu.get_barrier_semaphore(), DEV - 1)


def await_bytes(part, sem):
    pltpu.make_async_copy(part, part, sem).wait()


def sent(src, send_sem):
    await_bytes(src.at[pl.ds(0, 5 * (DEV - 1))], send_sem)


def remote(src, dst, send_sem, recv_sem, to):
    return pltpu.make_async_remote_copy(
        src_ref=src, dst_ref=dst, send_sem=send_sem, recv_sem=recv_sem, device_id=to, device_id_type=MESH
    )


def gather_and_send(pick, x, stage, src, dst, send_sem, recv_sem, sign):
    left = iota((1, 128), 1) < VECS

    def fill(c):
        for u in range(8):
            for r in range(HALF):
                one = x[pl.ds(pick.at[r, pl.ds(16 * u, 16)][c], 1), :]
                two = x[pl.ds(pick.at[r + HALF, pl.ds(16 * u, 16)][c], 1), :]
                stage[u, r : r + 1, :] = jnp.where(left, one, two)
            for q in range(5):
                src[(c * 8 + u) * 5 + q] = stage[u, 4 * q : 4 * q + 4, :].astype(BF16)

    def send(c):
        for u, to in enumerate(group_of(c, sign)):
            i = c * 8 + u
            part = pl.ds(i * 5, 5)
            if isinstance(c, int) and i == DEV - 1:
                pltpu.make_async_copy(src.at[part], dst.at[part], recv_sem.at[c]).start()
            else:
                remote(src.at[part], dst.at[part], send_sem, recv_sem.at[c], to).start()

    fill(0)

    def loop(c, carry):
        send(c)
        fill(c + 1)
        return carry

    lax.fori_loop(0, 15, loop, 0)
    send(15)


def receive(arrived, recv_sem, y, groups=range(16)):
    for j in groups:
        await_bytes(arrived.at[pl.ds(40 * j, 40)], recv_sem.at[j])
        for i in range(8 * j, 8 * j + 8):
            for q in range(5):
                rows = arrived[5 * i + q].astype(F32)
                at = i * BLOCK + 4 * q
                y[at : at + 4, :] = rows
                y[DEV * BLOCK + at : DEV * BLOCK + at + 4, :] = pltpu.roll(rows, 64, 1)


def block(k):
    return slice((CROSS - 1 - k) * RANK, (CROSS - k) * RANK)


def above(k):
    return slice(0, (CROSS - 1 - k) * RANK)


def rows_of(j):
    return slice((5 - j) * RANK, (6 - j) * RANK)


def place():
    leaf, sub = lax.axis_index("leaf"), lax.axis_index("sub")
    return leaf // 4, lax.rem(leaf, 4), sub // 2, lax.rem(sub, 2)


def group(phase):
    x, z, y, core = place()
    leaf, sub = lax.axis_index("leaf"), lax.axis_index("sub")
    return [
        (2, core, None),
        (4, y, lambda m, c: {"leaf": leaf, "sub": m * 2 + c}),
        (4, z, lambda m, c: {"leaf": x * 4 + m, "sub": y * 2 + c}),
        (4, x, lambda m, c: {"leaf": m * 4 + z, "sub": y * 2 + c}),
    ][phase]


def share(phase, buf, send_sem, recv_sem, wait=False):
    members, me, target = group(phase)
    leaf, (x, z, y, core) = lax.axis_index("leaf"), place()
    others = buf.at[pl.ds(0, members - 1)]

    def copy_to(c, to):
        return remote(buf.at[me], buf.at[me], send_sem.at[phase, c], recv_sem.at[phase], to)

    if phase == 0:
        if not wait:
            copy_to(0, {"leaf": leaf, "sub": y * 2 + 1 - core}).start()
        else:
            await_bytes(others, send_sem.at[phase, 0])
    else:

        @pl.when(core == 1)
        def _():
            for c in range(2):
                if wait:
                    await_bytes(others, send_sem.at[phase, c])
                    continue
                for i in (2, 1, 3):
                    copy_to(c, target(lax.rem(me + i, members), c)).start()

    if wait:
        await_bytes(others, recv_sem.at[phase])


def fold(a):
    return jnp.concatenate([a[:32], a[32:]], axis=1)


def unfold(a):
    return jnp.concatenate([a[:, :64], a[:, 64:]], axis=0)


def kernel(
    counts,
    codes_h,
    slots_h,
    vec_h,
    inverse_h,
    left_h,
    right_h,
    out_h,
    codes,
    slots_ref,
    vec,
    out,
    inverse,
    left,
    right,
    pick_v,
    pick,
    rank_ref,
    flat_v,
    flat,
    x,
    stage,
    pos_src,
    pos_dst,
    src1,
    dst1,
    src2,
    dst2,
    y,
    inv_v,
    inv,
    back_v,
    back,
    field,
    v_a,
    v_b,
    v_c,
    v_d,
    g_a,
    g_b,
    g_c,
    g_d,
    partner,
    g_l,
    near,
    load_sem,
    pos_sem,
    index_sem,
    send_sem,
    recv1,
    recv2,
    send_v,
    recv_v,
    send_g,
    recv_g,
):
    scale = [1.0 / math.sqrt(ROWS * 2**k) for k in range(CROSS)]
    with jax.named_scope("enter"):
        loads = [
            pltpu.make_async_copy(h, v, load_sem.at[i])
            for i, (h, v) in enumerate(
                (
                    (codes_h, codes),
                    (slots_h, slots_ref),
                    (vec_h, vec),
                    (left_h, left),
                    (inverse_h, inverse),
                )
            )
        ]
        for load in loads[:3]:
            load.start()
        enter()
    with jax.named_scope("route"):
        loads[0].wait()
        loads[1].wait()
        for load in loads[3:]:
            load.start()
        for k in range(LEVELS):
            pltpu.make_async_copy(right_h.at[k], right.at[LEVELS - 1 - k], load_sem.at[5]).start()
        live, owner, ranks, base, total = route(counts, slots_ref, codes, rank_ref)
        rows = jnp.where(live, bucket_row(owner, ranks), 0).astype(F32)
        rows = jnp.concatenate([rows, jnp.zeros((DEV - 40, 128), F32)], axis=0).T.astype(I32)
        flat_v[...] = jnp.clip(rows, 0, 2 * DEV * BLOCK - 1)
        both = total[:, :128].astype(I32)
        source = both * 128 + pltpu.roll(both, 64, 1)
        lane128 = iota((DEV, 128), 1)
        pick_v[...] = jnp.clip(source.astype(F32).T[:PEER].astype(I32), 0, SLOTS - 1)
        pick_copy = pltpu.make_async_copy(pick_v, pick, index_sem.at[0])
        pick_copy.start()
        flat_copy = pltpu.make_async_copy(flat_v, flat, index_sem.at[1])
        flat_copy.start()
        position = total[:, 128:]
        spot = position * 64.0 + pltpu.roll(position, 64, 1)
        pos_src[...] = jnp.where(lane128.astype(F32) < base, spot, float(ROWS)).reshape(DEV, 1, 128)
        pos_dst[DEV - 1] = pos_src[DEV - 1]
    with jax.named_scope("rows"):
        loads[2].wait()
        for a in range(40):
            part = vec[:, a * 128 : (a + 1) * 128].astype(F32)
            x[a * 128 : (a + 1) * 128, :] = jnp.concatenate([part, part], axis=0).T
        pick_copy.wait()
    with jax.named_scope("entered"):
        entered()
    with jax.named_scope("positions"):
        for c in range(16):
            for u, to in enumerate(group_of(c, 1)[: 8 if c < 15 else 7]):
                i = 16 * u + c
                remote(pos_src.at[i], pos_dst.at[i], pos_sem.at[0], pos_sem.at[1], to).start()
    with jax.named_scope("send"):
        gather_and_send(pick, x, stage, src1, dst1, send_sem.at[0], recv1, 1)
    with jax.named_scope("gram"):
        loads[3].wait()
        await_bytes(right, load_sem.at[5])
        sums = [None] * LOCAL
        cross = None
        for b in range(16):
            at = slice(b * LEAF, (b + 1) * LEAF)
            gram = dot_nt(
                left[: LEVELS - 1, :, at].reshape(10 * RANK, LEAF),
                right[: LEVELS - 1, :, at].reshape(10 * RANK, LEAF),
            )
            for j in range(LOCAL):
                part = gram[j * RANK : (j + 1) * RANK]
                sums[j] = part if b % 2**j == 0 else sums[j] + part
                if (b + 1) % 2**j == 0:
                    g_l[32 - 2 ** (5 - j) + b // 2**j, :, : 10 * RANK] = sums[j].astype(BF16)
            part = gram[LOCAL * RANK :, : CROSS * RANK]
            cross = part if b == 0 else cross + part
        core = group(0)[1]
        g_a[core] = jnp.zeros((192, 256), BF16)
        for j in range(CROSS - 1):
            g_a[core, rows_of(j), : CROSS * RANK] = cross[j * RANK : (j + 1) * RANK].astype(BF16)
        share(0, g_a, send_g, recv_g)
    with jax.named_scope("inv"):
        await_bytes(pos_dst.at[pl.ds(0, DEV - 1)], pos_sem.at[1])
        await_bytes(pos_src.at[pl.ds(0, DEV - 1)], pos_sem.at[0])
        spot = pos_dst[...].reshape(DEV, 128).astype(I32)
        back_v[...] = jnp.clip(spot.astype(F32).T[:PEER].astype(I32), 0, ROWS - 1)
        back_copy = pltpu.make_async_copy(back_v, back, index_sem.at[2])
        back_copy.start()
        high_t = (spot >> 6).astype(F32).T
        low_t = (spot & 63).astype(F32).T
        ids = iota((64, 128), 0).astype(F32)
        lanes = iota((64, 128), 1).astype(F32)
        found = jnp.zeros((64, 128), F32)

        def tables(r):
            hit = jnp.where(ids == high_t[r : r + 1, :], 1.0, 0.0).astype(BF16)
            match = ids == low_t[r : r + 1, :]
            table = [jnp.where(match, lanes, 0.0), jnp.where(match, float(r), 0.0)]
            return hit, jnp.concatenate(table, axis=0).astype(BF16)

        for r in range(0, PEER, 2):
            hits, parts = zip(tables(r), tables(r + 1))
            found = found + dot_nt(jnp.concatenate(hits, axis=1), jnp.concatenate(parts, axis=1))
        whole = found.astype(I32)
        inv_v[...] = jnp.clip(
            jnp.where(iota((64, 128), 1) < 64, bucket_row(whole, pltpu.roll(whole, 64, 1)), 0),
            0,
            2 * DEV * BLOCK - 1,
        )
        inv_copy = pltpu.make_async_copy(inv_v, inv, index_sem.at[3])
        inv_copy.start()
    with jax.named_scope("gram_y"):
        share(0, g_a, send_g, recv_g, wait=True)
        ysum = g_a[0].astype(F32) + g_a[1].astype(F32)
        mine = group(1)[1]
        g_b[mine, :160] = ysum[:160, :128].astype(BF16)
        g_b[mine, 160:] = ysum[128:160, 128:].astype(BF16)
    with jax.named_scope("receive"):
        receive(dst1, recv1, y, range(12))
        share(1, g_b, send_g, recv_g)
        receive(dst1, recv1, y, range(12, 16))
        inv_copy.wait()
    with jax.named_scope("tree"):

        def pull(c, carry):
            for u in range(128):
                at = pl.ds(u * 32 + c, 1)
                x[at, :] = y[pl.ds(inv.at[u // 2, pl.ds(u % 2 * 32, 32)][c], 1), :]
            return carry

        lax.fori_loop(0, 32, pull, 0)
    with jax.named_scope("leaf"):
        loads[4].wait()
        for l in range(ROWS // LEAF):
            at = slice(l * LEAF, (l + 1) * LEAF)
            field[:, at] = dot_nt(x[at, :].T[:VECS].astype(BF16), inverse[l])
    with jax.named_scope("gram_z"):
        share(1, g_b, send_g, recv_g, wait=True)
        zsum = (g_b[0, :96, :128].astype(F32) + g_b[1, :96, :128].astype(F32)) + (
            g_b[2, :96, :128].astype(F32) + g_b[3, :96, :128].astype(F32)
        )
        g_c[group(2)[1]] = zsum.astype(BF16)
        share(2, g_c, send_g, recv_g)
    with jax.named_scope("local"):
        vs = [
            dot_nt(
                field[:, b * LEAF : (b + 1) * LEAF].astype(BF16),
                right[:, :, b * LEAF : (b + 1) * LEAF].reshape(LEVELS * RANK, LEAF),
            )
            for b in range(16)
        ]
        for k in range(LOCAL):
            rest = (LEVELS - 1 - k) * RANK
            merged = []
            for m in range(len(vs) // 2):
                va, vb = vs[2 * m], vs[2 * m + 1]
                p2 = [
                    (v[:, rest : rest + RANK] * (1.0 / math.sqrt(LEAF * 2**k))).astype(BF16) for v in (vb, va)
                ]
                first = 32 - 2 ** (5 - k) + 2 * m
                g2 = jnp.concatenate([g_l[first, :, :rest], g_l[first + 1, :, :rest]], axis=0)
                merged.append(va[:, :rest] + vb[:, :rest] - dot(jnp.concatenate(p2, axis=1), g2))
                for n in range(2):
                    for b in range((2 * m + n) * 2**k, (2 * m + n + 1) * 2**k):
                        near[b, :, k * RANK : (k + 1) * RANK] = p2[n]
            vs = merged
        v = vs[0]

    def level_rows(k, g):
        if k == 1:
            return jnp.concatenate([g[128:160], g[160:]], axis=1)[:, above(1)]
        return g[rows_of(k), above(k)]

    def merge(k, va, vb, ga, gb):
        pa = (vb[:, block(k)] * scale[k]).astype(BF16)
        pb = (va[:, block(k)] * scale[k]).astype(BF16)
        if k == CROSS - 1:
            return pa, pb, None
        p2 = jnp.concatenate([pa, pb], axis=1)
        g2 = jnp.concatenate([level_rows(k, ga), level_rows(k, gb)], axis=0).astype(BF16)
        return pa, pb, va[:, above(k)] + vb[:, above(k)] - dot(p2, g2)

    def keep(k, p):
        partner[:, k * RANK : (k + 1) * RANK] = p

    with jax.named_scope("cross_core"):
        core = group(0)[1]
        v_a[core, :, 192:] = jnp.zeros((VECS, 64), F32)
        v_a[core, :, : CROSS * RANK] = v
        share(0, v_a, send_v, recv_v)
        share(0, v_a, send_v, recv_v, wait=True)
        pa, pb, v = merge(0, v_a[0], v_a[1], g_a[0], g_a[1])
        keep(0, jnp.where(core == 0, pa, pb))

    def four(phase, k, v, v_buf, g_buf):
        me = group(phase)[1]
        v = v.astype(BF16).astype(F32)
        if phase == 1:
            v_buf[me, :64] = v[:, :128].astype(BF16)
            v_buf[me, 64:] = fold(v[:, 128:]).astype(BF16)
        elif phase == 2:
            v_buf[me] = v.astype(BF16)
        else:
            v_buf[me] = fold(v).astype(BF16)
        share(phase, v_buf, send_v, recv_v)
        if phase == 1:
            share(2, g_c, send_g, recv_g, wait=True)
            xsum = (g_c[0, :32].astype(F32) + g_c[1, :32].astype(F32)) + (
                g_c[2, :32].astype(F32) + g_c[3, :32].astype(F32)
            )
            g_d[group(3)[1]] = xsum.astype(BF16)
            share(3, g_d, send_g, recv_g)
            for b in range(16):
                at = slice(b * LEAF, (b + 1) * LEAF)
                field[:, at] -= dot(near[b], left[:LOCAL, :, at].reshape(LOCAL * RANK, LEAF))
        share(phase, v_buf, send_v, recv_v, wait=True)
        vs = [v_buf[i].astype(F32) for i in range(4)]
        if phase == 1:
            vs = [jnp.concatenate([u[:64], unfold(u[64:])], axis=1) for u in vs]
        elif phase == 3:
            vs = [unfold(u) for u in vs]
        gs = [g_buf[i].astype(F32) for i in range(4)]
        p0, p1, v01 = merge(k, vs[0], vs[1], gs[0], gs[1])
        p2, p3, v23 = merge(k, vs[2], vs[3], gs[2], gs[3])
        keep(k, jnp.where(me < 2, jnp.where(me == 0, p0, p1), jnp.where(me == 2, p2, p3)))
        pa, pb, v = merge(k + 1, v01, v23, gs[0] + gs[1], gs[2] + gs[3])
        keep(k + 1, jnp.where(me < 2, pa, pb))
        return v

    with jax.named_scope("cross_y"):
        v = four(1, 1, v, v_b, g_b)
    with jax.named_scope("cross_z"):
        v = four(2, 3, v, v_c, g_c)
    with jax.named_scope("cross_x"):
        share(3, g_d, send_g, recv_g, wait=True)
        four(3, 5, v, v_d, g_d)
    with jax.named_scope("finish"):
        for c in range(16):
            at = slice(c * LEAF, (c + 1) * LEAF)
            done = field[:, at] - dot(
                partner[:, : CROSS * RANK], left[LOCAL:, :, at].reshape(CROSS * RANK, LEAF)
            )
            x[at, :] = jnp.concatenate([done, done], axis=0).T
        back_copy.wait()
        sent(src1, send_sem.at[0])
    with jax.named_scope("send_back"):
        gather_and_send(back, x, stage, src2, dst2, send_sem.at[1], recv2, -1)
    with jax.named_scope("receive_back"):
        flat_copy.wait()
        receive(dst2, recv2, y)
    with jax.named_scope("output"):
        alive = jnp.where(live_slots(counts, slots_ref[...]), 1, 0)

        slots_ref[...] = alive

        def pull_slots(a):
            for u in range(128):
                x[pl.ds(pl.multiple_of(a * 128, 128) + u, 1), :] = y[pl.ds(flat.at[u][a], 1), :]

        def push(a):
            at = pl.multiple_of(a * 128, 128)
            part = x[pl.ds(at, 128), :].T[:VECS]
            out[:, pl.ds(at, 128)] = jnp.where(slots_ref[pl.ds(a, 1), :] > 0, part, 0.0).astype(BF16)

        pull_slots(0)
        pull_slots(1)

        def next_slots(c, carry):
            push(2 * c)
            push(2 * c + 1)
            pull_slots(2 * c + 2)
            pull_slots(2 * c + 3)
            return carry

        stores = []
        for part in range(4):
            lax.fori_loop(5 * part, 5 * part + 5 - part // 3, next_slots, 0)
            if part == 3:
                push(38)
                push(39)
            at = pl.ds(part * 1280, 1280)
            store = pltpu.make_async_copy(out.at[:, at], out_h.at[:, at], load_sem.at[part])
            store.start()
            stores.append(store)
        for store in stores:
            store.wait()
        sent(src2, send_sem.at[1])


def body(vectors, row_counts, tree_slot, leaf_inverse, left_basis, right_basis):
    anywhere = pl.BlockSpec(memory_space=pl.ANY)
    dma = pltpu.SemaphoreType.DMA
    blocks = pltpu.VMEM((DEV * 5, 4, 128), BF16)
    return pl.pallas_call(
        kernel,
        out_shape=jax.ShapeDtypeStruct((VECS, SLOTS), BF16),
        in_specs=[SMEM] + [anywhere] * 6,
        out_specs=anywhere,
        scratch_shapes=[
            pltpu.VMEM((DEV, 128), I32),
            pltpu.VMEM((40, 128), I32),
            pltpu.VMEM((VECS, SLOTS), BF16),
            pltpu.VMEM((VECS, SLOTS), BF16),
            pltpu.VMEM(leaf_inverse.shape, BF16),
            pltpu.VMEM(left_basis.shape, BF16),
            pltpu.VMEM(right_basis.shape, BF16),
            pltpu.VMEM((PEER, DEV), I32),
            pltpu.SMEM((PEER, DEV), I32),
            pltpu.VMEM((40, 128), F32),
            pltpu.VMEM((DEV, 128), I32),
            pltpu.SMEM((DEV, 128), I32),
            pltpu.VMEM((SLOTS, 128), F32),
            pltpu.VMEM((8, BLOCK, 128), F32),
            pltpu.VMEM((DEV, 1, 128), F32),
            pltpu.VMEM((DEV, 1, 128), F32),
            blocks,
            blocks,
            blocks,
            blocks,
            pltpu.VMEM((2 * DEV * BLOCK, 128), F32),
            pltpu.VMEM((64, 128), I32),
            pltpu.SMEM((64, 128), I32),
            pltpu.VMEM((PEER, DEV), I32),
            pltpu.SMEM((PEER, DEV), I32),
            pltpu.VMEM((VECS, ROWS), F32),
            pltpu.VMEM((2, VECS, 256), F32),
            pltpu.VMEM((4, 96, 128), BF16),
            pltpu.VMEM((4, VECS, 128), BF16),
            pltpu.VMEM((4, 32, 128), BF16),
            pltpu.VMEM((2, 192, 256), BF16),
            pltpu.VMEM((4, 192, 128), BF16),
            pltpu.VMEM((4, 96, 128), BF16),
            pltpu.VMEM((4, 32, 128), BF16),
            pltpu.VMEM((VECS, 256), BF16),
            pltpu.VMEM((30, RANK, 384), BF16),
            pltpu.VMEM((16, VECS, LOCAL * RANK), BF16),
            dma((6,)),
            dma((2,)),
            dma((4,)),
            dma((2,)),
            dma((16,)),
            dma((16,)),
            dma((4, 2)),
            dma((4,)),
            dma((4, 2)),
            dma((4,)),
        ],
        compiler_params=pltpu.CompilerParams(collective_id=0, has_side_effects=True),
        name="apply",
    )(
        row_counts,
        jnp.asarray(np.repeat(CODES[:, None], 128, 1)),
        tree_slot.reshape(40, 128), vectors, leaf_inverse, left_basis, right_basis)


def solution(mesh):
    both = ("leaf", "sub")
    return jax.shard_map(
        body,
        mesh=mesh,
        in_specs=(
            P(None, both),
            P(),
            P(both),
            P(both, None, None),
            P(None, None, both),
            P(None, None, both),
        ),
        out_specs=P(None, both),
        check_vma=False,
    )
```

```python
import functools
import math

import jax
import jax.numpy as jnp
import numpy as np
from jax import lax
from jax.experimental import pallas as pl
from jax.experimental.pallas import tpu as pltpu
from jax.sharding import PartitionSpec as P

DEV = 128
PEER = 40
HALF = 20
BLOCK = 20
ROWS = 4096
SLOTS = 5120
VECS = 64
LEAF = 256
RANK = 32
LOCAL = 4
CROSS = 7
LEVELS = 11
F32 = jnp.float32
BF16 = jnp.bfloat16
I32 = jnp.int32
VMEM = pl.BlockSpec(memory_space=pltpu.VMEM)
SMEM = pl.BlockSpec(memory_space=pltpu.SMEM)
NT = (((1,), (1,)), ((), ()))
MESH = pl.DeviceIdType.MESH


FAR = (2, 1, 3, 0)
PAIRS = sorted(((dx, dz) for dx in FAR for dz in FAR), key=lambda c: -sum(min(d, 4 - d) for d in c))
ORDER = [(dx, dy, dz, dc) for dx, dz in PAIRS for dy in FAR for dc in (1, 0)]
CODES = np.array([32 * dx + 8 * dz + 2 * dy + dc for dx, dy, dz, dc in ORDER], np.int32).reshape(16, 8).T.reshape(-1)


def place():
    leaf, sub = lax.axis_index("leaf"), lax.axis_index("sub")
    return leaf // 4, lax.rem(leaf, 4), sub // 2, lax.rem(sub, 2)


def wrapped(at, d):
    return lax.rem(at + 4 + d, 4)


def chosen(n, values):
    value = values[0]
    for k in range(1, len(values)):
        value = jnp.where(n == k, values[k], value)
    return value


def group_of(c, sign):
    x, z, y, core = place()
    if isinstance(c, int):
        dx, dz = PAIRS[c]
    else:
        dx, dz = chosen(c, [p[0] for p in PAIRS]), chosen(c, [p[1] for p in PAIRS])
    leaf = wrapped(x, sign * dx) * 4 + wrapped(z, sign * dz)
    return [{"leaf": leaf, "sub": wrapped(y, sign * dy) * 2 + pc} for dy in FAR for pc in (1 - core, core)]


def iota(shape, dim):
    return lax.broadcasted_iota(I32, shape, dim)


def dot_nt(a, b):
    return lax.dot_general(a, b, NT, preferred_element_type=F32)


def dot(a, b):
    return jnp.dot(a, b, preferred_element_type=F32)


def bucket_row(label, rank):
    owner = (label & 15) * 8 + (label >> 4)
    return jnp.where(rank < HALF, owner * BLOCK + rank, DEV * BLOCK + owner * BLOCK + rank - HALF)


def live_slots(counts, slots):
    index = iota((40, 128), 0) * 128 + iota((40, 128), 1)
    mine = lax.axis_index("leaf") * 8 + lax.axis_index("sub")
    return (index < counts[mine]) & (slots >= 0)


def route(counts, slots_ref, codes, rank_ref):
    slots = slots_ref[...]
    live = live_slots(counts, slots)
    x, z, y, core = place()
    away = (
        (((slots >> 17) + 4 - x) & 3) * 32
        + (((slots >> 15) + 4 - z) & 3) * 8
        + (((slots >> 13) + 4 - y) & 3) * 2
        + (((slots >> 12) + 2 - core) & 1)
    )
    owner = jnp.where(live, away, DEV)
    high = ((slots & 4095) >> 6).astype(F32)
    low = (slots & 63).astype(F32)
    ids = codes[...]
    before = jnp.where(iota((128, 256), 0) < iota((128, 256), 1), 1.0, 0.0).astype(BF16)
    start = (iota((DEV, 128), 0) * 64).astype(F32)
    base = start
    for a in range(40):
        hit = ids == owner[a : a + 1, :]
        earlier = dot(jnp.where(hit, 1.0, 0.0).astype(BF16), before)
        rank_ref[a : a + 1, :] = jnp.sum(jnp.where(hit, base + earlier[:, :128], 0.0), axis=0, keepdims=True)
        base = base + earlier[:, 128:]
    found = rank_ref[...].astype(I32)
    ranks = found & 63
    r64 = iota((64, 128), 0)
    lane = iota((64, 128), 1).astype(F32)
    total = jnp.zeros((DEV, 256), F32)
    def tables(a):
        hit = jnp.where(ids == owner[a : a + 1, :], 1.0, 0.0).astype(BF16)
        match = r64 == ranks[a : a + 1, :]
        table = jnp.concatenate(
            [
                jnp.where(match, float(a), 0.0),
                jnp.where(match, lane, 0.0),
                jnp.where(match, high[a : a + 1, :], 0.0),
                jnp.where(match, low[a : a + 1, :], 0.0),
            ],
            axis=0,
        ).astype(BF16)
        return hit, table

    for a in range(0, 40, 2):
        hits, parts = zip(tables(a), tables(a + 1))
        total = total + dot_nt(jnp.concatenate(hits, axis=1), jnp.concatenate(parts, axis=1))
    return live, found >> 6, ranks, base - start, total


def enter():
    barrier = pltpu.get_barrier_semaphore()
    for c in range(16):
        for to in group_of(c, 1)[: 8 if c < 15 else 7]:
            pl.semaphore_signal(barrier, 1, device_id=to, device_id_type=MESH)


def entered():
    pl.semaphore_wait(pltpu.get_barrier_semaphore(), DEV - 1)


def await_bytes(part, sem):
    pltpu.make_async_copy(part, part, sem).wait()


def sent(src, send_sem):
    await_bytes(src.at[pl.ds(0, 5 * (DEV - 1))], send_sem)


def remote(src, dst, send_sem, recv_sem, to):
    return pltpu.make_async_remote_copy(
        src_ref=src, dst_ref=dst, send_sem=send_sem, recv_sem=recv_sem, device_id=to, device_id_type=MESH
    )


def gather_and_send(pick, x, stage, src, dst, send_sem, recv_sem, sign):
    left = iota((1, 128), 1) < VECS

    def fill(c):
        for u in range(8):
            for r in range(HALF):
                one = x[pl.ds(pick.at[r, pl.ds(16 * u, 16)][c], 1), :]
                two = x[pl.ds(pick.at[r + HALF, pl.ds(16 * u, 16)][c], 1), :]
                stage[u, r : r + 1, :] = jnp.where(left, one, two)
            for q in range(5):
                src[(c * 8 + u) * 5 + q] = stage[u, 4 * q : 4 * q + 4, :].astype(BF16)

    def send(c):
        for u, to in enumerate(group_of(c, sign)):
            i = c * 8 + u
            part = pl.ds(i * 5, 5)
            if isinstance(c, int) and i == DEV - 1:
                pltpu.make_async_copy(src.at[part], dst.at[part], recv_sem.at[c]).start()
            else:
                remote(src.at[part], dst.at[part], send_sem, recv_sem.at[c], to).start()

    fill(0)

    def loop(c, carry):
        send(c)
        fill(c + 1)
        return carry

    lax.fori_loop(0, 15, loop, 0)
    send(15)


def receive(arrived, recv_sem, y, groups=range(16)):
    for j in groups:
        await_bytes(arrived.at[pl.ds(40 * j, 40)], recv_sem.at[j])
        for i in range(8 * j, 8 * j + 8):
            for q in range(5):
                rows = arrived[5 * i + q].astype(F32)
                at = i * BLOCK + 4 * q
                y[at : at + 4, :] = rows
                y[DEV * BLOCK + at : DEV * BLOCK + at + 4, :] = pltpu.roll(rows, 64, 1)


def block(k):
    return slice((CROSS - 1 - k) * RANK, (CROSS - k) * RANK)


def above(k):
    return slice(0, (CROSS - 1 - k) * RANK)


def rows_of(j):
    return slice((5 - j) * RANK, (6 - j) * RANK)


def place():
    leaf, sub = lax.axis_index("leaf"), lax.axis_index("sub")
    return leaf // 4, lax.rem(leaf, 4), sub // 2, lax.rem(sub, 2)


def group(phase):
    x, z, y, core = place()
    leaf, sub = lax.axis_index("leaf"), lax.axis_index("sub")
    return [
        (2, core, lambda m: {"leaf": leaf, "sub": y * 2 + m}),
        (4, y, lambda m: {"leaf": leaf, "sub": m * 2 + core}),
        (4, z, lambda m: {"leaf": x * 4 + m, "sub": sub}),
        (4, x, lambda m: {"leaf": m * 4 + z, "sub": sub}),
    ][phase]


def share(phase, buf, send_sem, recv_sem, wait=False):
    members, me, target = group(phase)
    others = buf.at[pl.ds(0, members - 1)]
    if wait:
        await_bytes(others, send_sem.at[phase])
        await_bytes(others, recv_sem.at[phase])
        return
    for i in (1,) if members == 2 else (2, 1, 3):
        to = target(lax.rem(me + i, members))
        remote(buf.at[me], buf.at[me], send_sem.at[phase], recv_sem.at[phase], to).start()


def fold(a):
    return jnp.concatenate([a[:32], a[32:]], axis=1)


def unfold(a):
    return jnp.concatenate([a[:, :64], a[:, 64:]], axis=0)


def kernel(
    counts,
    codes_h,
    slots_h,
    vec_h,
    inverse_h,
    left_h,
    right_h,
    out_h,
    codes,
    slots_ref,
    vec,
    out,
    inverse,
    left,
    right,
    pick_v,
    pick,
    rank_ref,
    flat_v,
    flat,
    x,
    stage,
    pos_src,
    pos_dst,
    src1,
    dst1,
    src2,
    dst2,
    y,
    inv_v,
    inv,
    back_v,
    back,
    field,
    v_a,
    v_b,
    v_c,
    v_d,
    g_a,
    g_b,
    g_c,
    g_d,
    partner,
    g_l,
    near,
    load_sem,
    pos_sem,
    part_sem,
    index_sem,
    send_sem,
    recv1,
    recv2,
    send_v,
    recv_v,
    send_g,
    recv_g,
):
    scale = [1.0 / math.sqrt(ROWS * 2**k) for k in range(CROSS)]
    with jax.named_scope("enter"):
        loads = [
            pltpu.make_async_copy(h, v, load_sem.at[i])
            for i, (h, v) in enumerate(
                (
                    (codes_h, codes),
                    (slots_h, slots_ref),
                    (vec_h, vec),
                    (left_h, left),
                    (inverse_h, inverse),
                )
            )
        ]
        for load in loads[:3]:
            load.start()
        enter()
    with jax.named_scope("route"):
        loads[0].wait()
        loads[1].wait()
        for load in loads[3:]:
            load.start()
        for k in range(LEVELS):
            pltpu.make_async_copy(right_h.at[k], right.at[LEVELS - 1 - k], load_sem.at[5]).start()
        live, owner, ranks, base, total = route(counts, slots_ref, codes, rank_ref)
        rows = jnp.where(live, bucket_row(owner, ranks), 0).astype(F32)
        rows = jnp.concatenate([rows, jnp.zeros((DEV - 40, 128), F32)], axis=0).T.astype(I32)
        flat_v[...] = jnp.clip(rows, 0, 2 * DEV * BLOCK - 1)
        both = total[:, :128].astype(I32)
        source = both * 128 + pltpu.roll(both, 64, 1)
        lane128 = iota((DEV, 128), 1)
        pick_v[...] = jnp.clip(source.astype(F32).T[:PEER].astype(I32), 0, SLOTS - 1)
        pick_copy = pltpu.make_async_copy(pick_v, pick, index_sem.at[0])
        pick_copy.start()
        flat_copy = pltpu.make_async_copy(flat_v, flat, index_sem.at[1])
        flat_copy.start()
        position = total[:, 128:]
        spot = position * 64.0 + pltpu.roll(position, 64, 1)
        pos_src[...] = jnp.where(lane128.astype(F32) < base, spot, float(ROWS)).reshape(DEV, 1, 128)
        pos_dst[DEV - 1] = pos_src[DEV - 1]
    with jax.named_scope("rows"):
        loads[2].wait()
        for a in range(40):
            part = vec[:, a * 128 : (a + 1) * 128].astype(F32)
            x[a * 128 : (a + 1) * 128, :] = jnp.concatenate([part, part], axis=0).T
        pick_copy.wait()
    with jax.named_scope("entered"):
        entered()
    with jax.named_scope("positions"):
        for c in range(16):
            for u, to in enumerate(group_of(c, 1)[: 8 if c < 15 else 7]):
                i = 16 * u + c
                remote(pos_src.at[i], pos_dst.at[i], pos_sem.at[0], pos_sem.at[1], to).start()
    with jax.named_scope("send"):
        gather_and_send(pick, x, stage, src1, dst1, send_sem.at[0], recv1, 1)
    with jax.named_scope("gram"):
        loads[3].wait()
        await_bytes(right, load_sem.at[5])
        sums = [None] * LOCAL
        cross = None
        for b in range(16):
            at = slice(b * LEAF, (b + 1) * LEAF)
            gram = dot_nt(
                left[: LEVELS - 1, :, at].reshape(10 * RANK, LEAF),
                right[: LEVELS - 1, :, at].reshape(10 * RANK, LEAF),
            )
            for j in range(LOCAL):
                part = gram[j * RANK : (j + 1) * RANK]
                sums[j] = part if b % 2**j == 0 else sums[j] + part
                if (b + 1) % 2**j == 0:
                    g_l[32 - 2 ** (5 - j) + b // 2**j, :, : 10 * RANK] = sums[j].astype(BF16)
            part = gram[LOCAL * RANK :, : CROSS * RANK]
            cross = part if b == 0 else cross + part
        core = group(0)[1]
        g_a[core] = jnp.zeros((192, 256), BF16)
        for j in range(CROSS - 1):
            g_a[core, rows_of(j), : CROSS * RANK] = cross[j * RANK : (j + 1) * RANK].astype(BF16)
        share(0, g_a, send_g, recv_g)
    with jax.named_scope("inv"):
        await_bytes(pos_dst.at[pl.ds(0, DEV - 1)], pos_sem.at[1])
        await_bytes(pos_src.at[pl.ds(0, DEV - 1)], pos_sem.at[0])
        spot = pos_dst[...].reshape(DEV, 128).astype(I32)
        back_v[...] = jnp.clip(spot.astype(F32).T[:PEER].astype(I32), 0, ROWS - 1)
        back_copy = pltpu.make_async_copy(back_v, back, index_sem.at[2])
        back_copy.start()
        high_t = (spot >> 6).astype(F32).T
        low_t = (spot & 63).astype(F32).T
        ids = iota((64, 128), 0).astype(F32)
        lanes = iota((64, 128), 1).astype(F32)
        found = jnp.zeros((64, 128), F32)

        def tables(r):
            hit = jnp.where(ids == high_t[r : r + 1, :], 1.0, 0.0).astype(BF16)
            match = ids == low_t[r : r + 1, :]
            table = [jnp.where(match, lanes, 0.0), jnp.where(match, float(r), 0.0)]
            return hit, jnp.concatenate(table, axis=0).astype(BF16)

        for r in range(0, PEER, 2):
            hits, parts = zip(tables(r), tables(r + 1))
            found = found + dot_nt(jnp.concatenate(hits, axis=1), jnp.concatenate(parts, axis=1))
        whole = found.astype(I32)
        inv_v[...] = jnp.clip(
            jnp.where(iota((64, 128), 1) < 64, bucket_row(whole, pltpu.roll(whole, 64, 1)), 0),
            0,
            2 * DEV * BLOCK - 1,
        )
        inv_copy = pltpu.make_async_copy(inv_v, inv, index_sem.at[3])
        inv_copy.start()
    with jax.named_scope("gram_y"):
        share(0, g_a, send_g, recv_g, wait=True)

        @pl.when(core == 1)
        def _():
            ysum = g_a[0].astype(F32) + g_a[1].astype(F32)
            mine = group(1)[1]
            g_b[mine, :160] = ysum[:160, :128].astype(BF16)
            g_b[mine, 160:] = ysum[128:160, 128:].astype(BF16)

    with jax.named_scope("receive"):
        receive(dst1, recv1, y, range(12))

        @pl.when(core == 1)
        def _():
            share(1, g_b, send_g, recv_g)

        receive(dst1, recv1, y, range(12, 16))
        inv_copy.wait()
    with jax.named_scope("tree"):

        def pull(c, carry):
            for u in range(128):
                at = pl.ds(u * 32 + c, 1)
                x[at, :] = y[pl.ds(inv.at[u // 2, pl.ds(u % 2 * 32, 32)][c], 1), :]
            return carry

        lax.fori_loop(0, 32, pull, 0)
    with jax.named_scope("leaf"):
        loads[4].wait()
        for l in range(ROWS // LEAF):
            at = slice(l * LEAF, (l + 1) * LEAF)
            field[:, at] = dot_nt(x[at, :].T[:VECS].astype(BF16), inverse[l])
    with jax.named_scope("gram_z"):

        @pl.when(core == 1)
        def _():
            share(1, g_b, send_g, recv_g, wait=True)
            zsum = (g_b[0, :96, :128].astype(F32) + g_b[1, :96, :128].astype(F32)) + (
                g_b[2, :96, :128].astype(F32) + g_b[3, :96, :128].astype(F32)
            )
            g_c[group(2)[1]] = zsum.astype(BF16)
            share(2, g_c, send_g, recv_g)

    with jax.named_scope("local"):
        vs = [
            dot_nt(
                field[:, b * LEAF : (b + 1) * LEAF].astype(BF16),
                right[:, :, b * LEAF : (b + 1) * LEAF].reshape(LEVELS * RANK, LEAF),
            )
            for b in range(16)
        ]
        for k in range(LOCAL):
            rest = (LEVELS - 1 - k) * RANK
            merged = []
            for m in range(len(vs) // 2):
                va, vb = vs[2 * m], vs[2 * m + 1]
                p2 = [
                    (v[:, rest : rest + RANK] * (1.0 / math.sqrt(LEAF * 2**k))).astype(BF16) for v in (vb, va)
                ]
                first = 32 - 2 ** (5 - k) + 2 * m
                g2 = jnp.concatenate([g_l[first, :, :rest], g_l[first + 1, :, :rest]], axis=0)
                merged.append(va[:, :rest] + vb[:, :rest] - dot(jnp.concatenate(p2, axis=1), g2))
                for n in range(2):
                    for b in range((2 * m + n) * 2**k, (2 * m + n + 1) * 2**k):
                        near[b, :, k * RANK : (k + 1) * RANK] = p2[n]
            vs = merged
        v = vs[0]

    def level_rows(k, g):
        if k == 1:
            return jnp.concatenate([g[128:160], g[160:]], axis=1)[:, above(1)]
        return g[rows_of(k), above(k)]

    def merge(k, va, vb, ga, gb):
        pa = (vb[:, block(k)] * scale[k]).astype(BF16)
        pb = (va[:, block(k)] * scale[k]).astype(BF16)
        if k == CROSS - 1:
            return pa, pb, None
        p2 = jnp.concatenate([pa, pb], axis=1)
        g2 = jnp.concatenate([level_rows(k, ga), level_rows(k, gb)], axis=0).astype(BF16)
        return pa, pb, va[:, above(k)] + vb[:, above(k)] - dot(p2, g2)

    with jax.named_scope("cross_core"):
        partner[:, 6 * RANK :] = jnp.zeros((VECS, 256 - 6 * RANK), BF16)
        v_a[core, :, 192:] = jnp.zeros((VECS, 64), F32)
        v_a[core, :, : CROSS * RANK] = v
        share(0, v_a, send_v, recv_v)
        share(0, v_a, send_v, recv_v, wait=True)
        mine = (v_a[1 - core, :, block(0)] * scale[0]).astype(BF16)

    def near_update():
        for b in range(16):
            at = slice(b * LEAF, (b + 1) * LEAF)
            field[:, at] -= dot(near[b], left[:LOCAL, :, at].reshape(LOCAL * RANK, LEAF)) + dot(
                mine, left[LOCAL, :, at]
            )

    def four(phase, k, v, v_buf, g_buf, meanwhile):
        me = group(phase)[1]
        if phase == 1:
            v_buf[me, :64] = v[:, :128].astype(BF16)
            v_buf[me, 64:] = fold(v[:, 128:]).astype(BF16)
        elif phase == 2:
            v_buf[me] = v.astype(BF16)
        else:
            v_buf[me] = fold(v).astype(BF16)
        share(phase, v_buf, send_v, recv_v)
        meanwhile()
        share(phase, v_buf, send_v, recv_v, wait=True)
        vs = [v_buf[i].astype(F32) for i in range(4)]
        if phase == 1:
            vs = [jnp.concatenate([u[:64], unfold(u[64:])], axis=1) for u in vs]
        elif phase == 3:
            vs = [unfold(u) for u in vs]
        gs = [g_buf[i].astype(F32) for i in range(4)]
        p0, p1, v01 = merge(k, vs[0], vs[1], gs[0], gs[1])
        p2, p3, v23 = merge(k, vs[2], vs[3], gs[2], gs[3])
        pa, pb, v = merge(k + 1, v01, v23, gs[0] + gs[1], gs[2] + gs[3])

        def keep():
            partner[:, (k - 1) * RANK : k * RANK] = jnp.where(
                me < 2, jnp.where(me == 0, p0, p1), jnp.where(me == 2, p2, p3)
            )
            partner[:, k * RANK : (k + 1) * RANK] = jnp.where(me < 2, pa, pb)

        return v, keep

    hand = remote(
        partner,
        partner,
        part_sem.at[0],
        part_sem.at[1],
        {"leaf": lax.axis_index("leaf"), "sub": lax.axis_index("sub") // 2 * 2},
    )
    with jax.named_scope("cross"):

        @pl.when(core == 1)
        def _():
            def first():
                share(2, g_c, send_g, recv_g, wait=True)
                xsum = (g_c[0, :32].astype(F32) + g_c[1, :32].astype(F32)) + (
                    g_c[2, :32].astype(F32) + g_c[3, :32].astype(F32)
                )
                g_d[group(3)[1]] = xsum.astype(BF16)
                share(3, g_d, send_g, recv_g)
                near_update()

            def last():
                keep()
                share(3, g_d, send_g, recv_g, wait=True)

            v = merge(0, v_a[0], v_a[1], g_a[0], g_a[1])[2]
            v, keep = four(1, 1, v, v_b, g_b, first)
            v, keep = four(2, 3, v, v_c, g_c, keep)
            v, keep = four(3, 5, v, v_d, g_d, last)
            keep()
            hand.start()
            hand.wait_send()

        @pl.when(core == 0)
        def _():
            near_update()
            hand.wait_recv()

    with jax.named_scope("finish"):
        for c in range(16):
            at = slice(c * LEAF, (c + 1) * LEAF)
            done = field[:, at] - dot(
                partner[:, : 6 * RANK], left[LOCAL + 1 :, :, at].reshape(6 * RANK, LEAF)
            )
            x[at, :] = jnp.concatenate([done, done], axis=0).T
        back_copy.wait()
        sent(src1, send_sem.at[0])
    with jax.named_scope("send_back"):
        gather_and_send(back, x, stage, src2, dst2, send_sem.at[1], recv2, -1)
    with jax.named_scope("receive_back"):
        flat_copy.wait()
        receive(dst2, recv2, y)
    with jax.named_scope("output"):
        alive = jnp.where(live_slots(counts, slots_ref[...]), 1, 0)

        slots_ref[...] = alive

        def pull_slots(a):
            for u in range(128):
                x[pl.ds(pl.multiple_of(a * 128, 128) + u, 1), :] = y[pl.ds(flat.at[u][a], 1), :]

        def push(a):
            at = pl.multiple_of(a * 128, 128)
            part = x[pl.ds(at, 128), :].T[:VECS]
            out[:, pl.ds(at, 128)] = jnp.where(slots_ref[pl.ds(a, 1), :] > 0, part, 0.0).astype(BF16)

        pull_slots(0)
        pull_slots(1)

        def next_slots(c, carry):
            push(2 * c)
            push(2 * c + 1)
            pull_slots(2 * c + 2)
            pull_slots(2 * c + 3)
            return carry

        stores = []
        for part in range(4):
            lax.fori_loop(5 * part, 5 * part + 5 - part // 3, next_slots, 0)
            if part == 3:
                push(38)
                push(39)
            at = pl.ds(part * 1280, 1280)
            store = pltpu.make_async_copy(out.at[:, at], out_h.at[:, at], load_sem.at[part])
            store.start()
            stores.append(store)
        for store in stores:
            store.wait()
        sent(src2, send_sem.at[1])


def body(vectors, row_counts, tree_slot, leaf_inverse, left_basis, right_basis):
    anywhere = pl.BlockSpec(memory_space=pl.ANY)
    outside = pl.BlockSpec(memory_space=pltpu.HBM)
    dma = pltpu.SemaphoreType.DMA
    blocks = pltpu.VMEM((DEV * 5, 4, 128), BF16)
    return pl.pallas_call(
        kernel,
        out_shape=jax.ShapeDtypeStruct((VECS, SLOTS), BF16),
        in_specs=[SMEM] + [outside] * 6,
        out_specs=anywhere,
        scratch_shapes=[
            pltpu.VMEM((DEV, 128), I32),
            pltpu.VMEM((40, 128), I32),
            pltpu.VMEM((VECS, SLOTS), BF16),
            pltpu.VMEM((VECS, SLOTS), BF16),
            pltpu.VMEM(leaf_inverse.shape, BF16),
            pltpu.VMEM(left_basis.shape, BF16),
            pltpu.VMEM(right_basis.shape, BF16),
            pltpu.VMEM((PEER, DEV), I32),
            pltpu.SMEM((PEER, DEV), I32),
            pltpu.VMEM((40, 128), F32),
            pltpu.VMEM((DEV, 128), I32),
            pltpu.SMEM((DEV, 128), I32),
            pltpu.VMEM((SLOTS, 128), F32),
            pltpu.VMEM((8, BLOCK, 128), F32),
            pltpu.VMEM((DEV, 1, 128), F32),
            pltpu.VMEM((DEV, 1, 128), F32),
            blocks,
            blocks,
            blocks,
            blocks,
            pltpu.VMEM((2 * DEV * BLOCK, 128), F32),
            pltpu.VMEM((64, 128), I32),
            pltpu.SMEM((64, 128), I32),
            pltpu.VMEM((PEER, DEV), I32),
            pltpu.SMEM((PEER, DEV), I32),
            pltpu.VMEM((VECS, ROWS), F32),
            pltpu.VMEM((2, VECS, 256), F32),
            pltpu.VMEM((4, 96, 128), BF16),
            pltpu.VMEM((4, VECS, 128), BF16),
            pltpu.VMEM((4, 32, 128), BF16),
            pltpu.VMEM((2, 192, 256), BF16),
            pltpu.VMEM((4, 192, 128), BF16),
            pltpu.VMEM((4, 96, 128), BF16),
            pltpu.VMEM((4, 32, 128), BF16),
            pltpu.VMEM((VECS, 256), BF16),
            pltpu.VMEM((30, RANK, 384), BF16),
            pltpu.VMEM((16, VECS, LOCAL * RANK), BF16),
            dma((6,)),
            dma((2,)),
            dma((2,)),
            dma((4,)),
            dma((2,)),
            dma((16,)),
            dma((16,)),
            dma((4,)),
            dma((4,)),
            dma((4,)),
            dma((4,)),
        ],
        compiler_params=pltpu.CompilerParams(
            collective_id=0, has_side_effects=True, vmem_limit_bytes=36 * 2**20
        ),
        name="apply",
    )(
        *(
            pltpu.with_memory_space_constraint(value, pltpu.HBM)
            for value in (
                row_counts,
                jnp.asarray(np.repeat(CODES[:, None], 128, 1)),
                tree_slot.reshape(40, 128),
                vectors,
                leaf_inverse,
                left_basis,
                right_basis,
            )
        ),
    )


def solution(mesh):
    both = ("leaf", "sub")
    return jax.shard_map(
        body,
        mesh=mesh,
        in_specs=(
            P(None, both),
            P(),
            P(both),
            P(both, None, None),
            P(None, None, both),
            P(None, None, both),
        ),
        out_specs=P(None, both),
        check_vma=False,
    )
```

```python
import functools
import math

import jax
import jax.numpy as jnp
import numpy as np
from jax import lax
from jax.experimental import pallas as pl
from jax.experimental.pallas import tpu as pltpu
from jax.sharding import PartitionSpec as P

DEV = 128
PEER = 40
HALF = 20
BLOCK = 20
ROWS = 4096
SLOTS = 5120
VECS = 64
LEAF = 256
RANK = 32
LOCAL = 4
CROSS = 7
LEVELS = 11
F32 = jnp.float32
BF16 = jnp.bfloat16
I32 = jnp.int32
VMEM = pl.BlockSpec(memory_space=pltpu.VMEM)
SMEM = pl.BlockSpec(memory_space=pltpu.SMEM)
NT = (((1,), (1,)), ((), ()))
MESH = pl.DeviceIdType.MESH


FAR = (2, 1, 3, 0)
PAIRS = sorted(((dx, dz) for dx in FAR for dz in FAR), key=lambda c: -sum(min(d, 4 - d) for d in c))
ORDER = [(dx, dy, dz, dc) for dx, dz in PAIRS for dy in FAR for dc in (1, 0)]
CODES = np.array([32 * dx + 8 * dz + 2 * dy + dc for dx, dy, dz, dc in ORDER], np.int32).reshape(16, 8).T.reshape(-1)


def place():
    leaf, sub = lax.axis_index("leaf"), lax.axis_index("sub")
    return leaf // 4, lax.rem(leaf, 4), sub // 2, lax.rem(sub, 2)


def wrapped(at, d):
    return lax.rem(at + 4 + d, 4)


def chosen(n, values):
    value = values[0]
    for k in range(1, len(values)):
        value = jnp.where(n == k, values[k], value)
    return value


def group_of(c, sign):
    x, z, y, core = place()
    if isinstance(c, int):
        dx, dz = PAIRS[c]
    else:
        dx, dz = chosen(c, [p[0] for p in PAIRS]), chosen(c, [p[1] for p in PAIRS])
    leaf = wrapped(x, sign * dx) * 4 + wrapped(z, sign * dz)
    return [{"leaf": leaf, "sub": wrapped(y, sign * dy) * 2 + pc} for dy in FAR for pc in (1 - core, core)]


def iota(shape, dim):
    return lax.broadcasted_iota(I32, shape, dim)


def dot_nt(a, b):
    return lax.dot_general(a, b, NT, preferred_element_type=F32)


def dot(a, b):
    return jnp.dot(a, b, preferred_element_type=F32)


def bucket_row(label, rank):
    owner = (label & 15) * 8 + (label >> 4)
    return jnp.where(rank < HALF, owner * BLOCK + rank, DEV * BLOCK + owner * BLOCK + rank - HALF)


def live_slots(counts, slots):
    index = iota((40, 128), 0) * 128 + iota((40, 128), 1)
    mine = lax.axis_index("leaf") * 8 + lax.axis_index("sub")
    return (index < counts[mine]) & (slots >= 0)


def route(counts, slots_ref, codes, rank_ref):
    slots = slots_ref[...]
    live = live_slots(counts, slots)
    x, z, y, core = place()
    away = (
        (((slots >> 17) + 4 - x) & 3) * 32
        + (((slots >> 15) + 4 - z) & 3) * 8
        + (((slots >> 13) + 4 - y) & 3) * 2
        + (((slots >> 12) + 2 - core) & 1)
    )
    owner = jnp.where(live, away, DEV)
    high = ((slots & 4095) >> 6).astype(F32)
    low = (slots & 63).astype(F32)
    ids = codes[...]
    before = jnp.where(iota((128, 256), 0) < iota((128, 256), 1), 1.0, 0.0).astype(BF16)
    start = (iota((DEV, 128), 0) * 64).astype(F32)
    base = start
    for a in range(40):
        hit = ids == owner[a : a + 1, :]
        earlier = dot(jnp.where(hit, 1.0, 0.0).astype(BF16), before)
        rank_ref[a : a + 1, :] = jnp.sum(jnp.where(hit, base + earlier[:, :128], 0.0), axis=0, keepdims=True)
        base = base + earlier[:, 128:]
    found = rank_ref[...].astype(I32)
    ranks = found & 63
    r64 = iota((64, 128), 0)
    lane = iota((64, 128), 1).astype(F32)
    total = jnp.zeros((DEV, 256), F32)
    def tables(a):
        hit = jnp.where(ids == owner[a : a + 1, :], 1.0, 0.0).astype(BF16)
        match = r64 == ranks[a : a + 1, :]
        table = jnp.concatenate(
            [
                jnp.where(match, float(a), 0.0),
                jnp.where(match, lane, 0.0),
                jnp.where(match, high[a : a + 1, :], 0.0),
                jnp.where(match, low[a : a + 1, :], 0.0),
            ],
            axis=0,
        ).astype(BF16)
        return hit, table

    for a in range(0, 40, 2):
        hits, parts = zip(tables(a), tables(a + 1))
        total = total + dot_nt(jnp.concatenate(hits, axis=1), jnp.concatenate(parts, axis=1))
    return live, found >> 6, ranks, base - start, total


def enter():
    barrier = pltpu.get_barrier_semaphore()
    for c in range(16):
        for to in group_of(c, 1)[: 8 if c < 15 else 7]:
            pl.semaphore_signal(barrier, 1, device_id=to, device_id_type=MESH)


def entered():
    pl.semaphore_wait(pltpu.get_barrier_semaphore(), DEV - 1)


def await_bytes(part, sem):
    pltpu.make_async_copy(part, part, sem).wait()


def sent(src, send_sem):
    await_bytes(src.at[pl.ds(0, 5 * (DEV - 1))], send_sem)


def remote(src, dst, send_sem, recv_sem, to):
    return pltpu.make_async_remote_copy(
        src_ref=src, dst_ref=dst, send_sem=send_sem, recv_sem=recv_sem, device_id=to, device_id_type=MESH
    )


def gather_and_send(pick, x, stage, src, dst, send_sem, recv_sem, sign):
    left = iota((1, 128), 1) < VECS

    def fill(c):
        for u in range(8):
            for r in range(HALF):
                one = x[pl.ds(pick.at[r, pl.ds(16 * u, 16)][c], 1), :]
                two = x[pl.ds(pick.at[r + HALF, pl.ds(16 * u, 16)][c], 1), :]
                stage[u, r : r + 1, :] = jnp.where(left, one, two)
            for q in range(5):
                src[(c * 8 + u) * 5 + q] = stage[u, 4 * q : 4 * q + 4, :].astype(BF16)

    def send(c):
        for u, to in enumerate(group_of(c, sign)):
            i = c * 8 + u
            part = pl.ds(i * 5, 5)
            if isinstance(c, int) and i == DEV - 1:
                pltpu.make_async_copy(src.at[part], dst.at[part], recv_sem.at[c]).start()
            else:
                remote(src.at[part], dst.at[part], send_sem, recv_sem.at[c], to).start()

    fill(0)

    def loop(c, carry):
        send(c)
        fill(c + 1)
        return carry

    lax.fori_loop(0, 15, loop, 0)
    send(15)


def receive(arrived, recv_sem, y, groups=range(16)):
    for j in groups:
        await_bytes(arrived.at[pl.ds(40 * j, 40)], recv_sem.at[j])
        for i in range(8 * j, 8 * j + 8):
            for q in range(5):
                rows = arrived[5 * i + q].astype(F32)
                at = i * BLOCK + 4 * q
                y[at : at + 4, :] = rows
                y[DEV * BLOCK + at : DEV * BLOCK + at + 4, :] = pltpu.roll(rows, 64, 1)


def block(k):
    return slice((CROSS - 1 - k) * RANK, (CROSS - k) * RANK)


def above(k):
    return slice(0, (CROSS - 1 - k) * RANK)


def rows_of(j):
    return slice((5 - j) * RANK, (6 - j) * RANK)


def place():
    leaf, sub = lax.axis_index("leaf"), lax.axis_index("sub")
    return leaf // 4, lax.rem(leaf, 4), sub // 2, lax.rem(sub, 2)


def group(phase):
    x, z, y, core = place()
    leaf, sub = lax.axis_index("leaf"), lax.axis_index("sub")
    return [
        (2, core, lambda m: {"leaf": leaf, "sub": y * 2 + m}),
        (4, y, lambda m: {"leaf": leaf, "sub": m * 2 + core}),
        (4, z, lambda m: {"leaf": x * 4 + m, "sub": sub}),
        (4, x, lambda m: {"leaf": m * 4 + z, "sub": sub}),
    ][phase]


def share(phase, buf, send_sem, recv_sem, wait=False):
    members, me, target = group(phase)
    others = buf.at[pl.ds(0, members - 1)]
    if wait:
        await_bytes(others, send_sem.at[phase])
        await_bytes(others, recv_sem.at[phase])
        return
    for i in (1,) if members == 2 else (2, 1, 3):
        to = target(lax.rem(me + i, members))
        remote(buf.at[me], buf.at[me], send_sem.at[phase], recv_sem.at[phase], to).start()


def fold(a):
    return jnp.concatenate([a[:32], a[32:]], axis=1)


def unfold(a):
    return jnp.concatenate([a[:, :64], a[:, 64:]], axis=0)


def kernel(
    counts,
    codes_h,
    slots_h,
    vec_h,
    inverse_h,
    left_h,
    right_h,
    out,
    codes,
    slots_ref,
    vec,
    inverse,
    left,
    right,
    pick_v,
    pick,
    rank_ref,
    flat_v,
    flat,
    x,
    stage,
    pos_src,
    pos_dst,
    src1,
    dst1,
    src2,
    dst2,
    y,
    inv_v,
    inv,
    back_v,
    back,
    field,
    v_a,
    v_b,
    v_c,
    v_d,
    g_a,
    g_b,
    g_c,
    g_d,
    partner,
    g_l,
    near,
    load_sem,
    pos_sem,
    part_sem,
    index_sem,
    send_sem,
    recv1,
    recv2,
    send_v,
    recv_v,
    send_g,
    recv_g,
):
    scale = [1.0 / math.sqrt(ROWS * 2**k) for k in range(CROSS)]
    with jax.named_scope("enter"):
        loads = [
            pltpu.make_async_copy(h, v, load_sem.at[i])
            for i, (h, v) in enumerate(
                (
                    (codes_h, codes),
                    (slots_h, slots_ref),
                    (vec_h, vec),
                    (left_h, left),
                    (inverse_h, inverse),
                )
            )
        ]
        for load in loads[:3]:
            load.start()
        enter()
    with jax.named_scope("route"):
        loads[0].wait()
        loads[1].wait()
        for load in loads[3:]:
            load.start()
        for k in range(LEVELS):
            pltpu.make_async_copy(right_h.at[k], right.at[LEVELS - 1 - k], load_sem.at[5]).start()
        live, owner, ranks, base, total = route(counts, slots_ref, codes, rank_ref)
        rows = jnp.where(live, bucket_row(owner, ranks), 0).astype(F32)
        rows = jnp.concatenate([rows, jnp.zeros((DEV - 40, 128), F32)], axis=0).T.astype(I32)
        flat_v[...] = jnp.clip(rows, 0, 2 * DEV * BLOCK - 1)
        both = total[:, :128].astype(I32)
        source = both * 128 + pltpu.roll(both, 64, 1)
        lane128 = iota((DEV, 128), 1)
        pick_v[...] = jnp.clip(source.astype(F32).T[:PEER].astype(I32), 0, SLOTS - 1)
        pick_copy = pltpu.make_async_copy(pick_v, pick, index_sem.at[0])
        pick_copy.start()
        flat_copy = pltpu.make_async_copy(flat_v, flat, index_sem.at[1])
        flat_copy.start()
        position = total[:, 128:]
        spot = position * 64.0 + pltpu.roll(position, 64, 1)
        pos_src[...] = jnp.where(lane128.astype(F32) < base, spot, float(ROWS)).reshape(DEV, 1, 128)
        pos_dst[DEV - 1] = pos_src[DEV - 1]
    with jax.named_scope("rows"):
        loads[2].wait()
        for a in range(40):
            part = vec[:, a * 128 : (a + 1) * 128].astype(F32)
            x[a * 128 : (a + 1) * 128, :] = jnp.concatenate([part, part], axis=0).T
        pick_copy.wait()
    with jax.named_scope("entered"):
        entered()
    with jax.named_scope("positions"):
        for c in range(16):
            for u, to in enumerate(group_of(c, 1)[: 8 if c < 15 else 7]):
                i = 16 * u + c
                remote(pos_src.at[i], pos_dst.at[i], pos_sem.at[0], pos_sem.at[1], to).start()
    with jax.named_scope("send"):
        gather_and_send(pick, x, stage, src1, dst1, send_sem.at[0], recv1, 1)
    with jax.named_scope("gram"):
        loads[3].wait()
        await_bytes(right, load_sem.at[5])
        sums = [None] * LOCAL
        cross = None
        for b in range(16):
            at = slice(b * LEAF, (b + 1) * LEAF)
            gram = dot_nt(
                left[: LEVELS - 1, :, at].reshape(10 * RANK, LEAF),
                right[: LEVELS - 1, :, at].reshape(10 * RANK, LEAF),
            )
            for j in range(LOCAL):
                part = gram[j * RANK : (j + 1) * RANK]
                sums[j] = part if b % 2**j == 0 else sums[j] + part
                if (b + 1) % 2**j == 0:
                    g_l[32 - 2 ** (5 - j) + b // 2**j, :, : 10 * RANK] = sums[j].astype(BF16)
            part = gram[LOCAL * RANK :, : CROSS * RANK]
            cross = part if b == 0 else cross + part
        core = group(0)[1]
        g_a[core] = jnp.zeros((192, 256), BF16)
        for j in range(CROSS - 1):
            g_a[core, rows_of(j), : CROSS * RANK] = cross[j * RANK : (j + 1) * RANK].astype(BF16)
        share(0, g_a, send_g, recv_g)
    with jax.named_scope("inv"):
        await_bytes(pos_dst.at[pl.ds(0, DEV - 1)], pos_sem.at[1])
        await_bytes(pos_src.at[pl.ds(0, DEV - 1)], pos_sem.at[0])
        spot = pos_dst[...].reshape(DEV, 128).astype(I32)
        back_v[...] = jnp.clip(spot.astype(F32).T[:PEER].astype(I32), 0, ROWS - 1)
        back_copy = pltpu.make_async_copy(back_v, back, index_sem.at[2])
        back_copy.start()
        high_t = (spot >> 6).astype(F32).T
        low_t = (spot & 63).astype(F32).T
        ids = iota((64, 128), 0).astype(F32)
        lanes = iota((64, 128), 1).astype(F32)
        found = jnp.zeros((64, 128), F32)

        def tables(r):
            hit = jnp.where(ids == high_t[r : r + 1, :], 1.0, 0.0).astype(BF16)
            match = ids == low_t[r : r + 1, :]
            table = [jnp.where(match, lanes, 0.0), jnp.where(match, float(r), 0.0)]
            return hit, jnp.concatenate(table, axis=0).astype(BF16)

        for r in range(0, PEER, 2):
            hits, parts = zip(tables(r), tables(r + 1))
            found = found + dot_nt(jnp.concatenate(hits, axis=1), jnp.concatenate(parts, axis=1))
        whole = found.astype(I32)
        inv_v[...] = jnp.clip(
            jnp.where(iota((64, 128), 1) < 64, bucket_row(whole, pltpu.roll(whole, 64, 1)), 0),
            0,
            2 * DEV * BLOCK - 1,
        )
        inv_copy = pltpu.make_async_copy(inv_v, inv, index_sem.at[3])
        inv_copy.start()
    with jax.named_scope("gram_y"):
        share(0, g_a, send_g, recv_g, wait=True)

        @pl.when(core == 1)
        def _():
            ysum = g_a[0].astype(F32) + g_a[1].astype(F32)
            mine = group(1)[1]
            g_b[mine, :160] = ysum[:160, :128].astype(BF16)
            g_b[mine, 160:] = ysum[128:160, 128:].astype(BF16)

    with jax.named_scope("receive"):
        receive(dst1, recv1, y, range(12))

        @pl.when(core == 1)
        def _():
            share(1, g_b, send_g, recv_g)

        receive(dst1, recv1, y, range(12, 16))
        inv_copy.wait()
    with jax.named_scope("tree"):

        def pull(c, carry):
            for u in range(128):
                at = pl.ds(u * 32 + c, 1)
                x[at, :] = y[pl.ds(inv.at[u // 2, pl.ds(u % 2 * 32, 32)][c], 1), :]
            return carry

        lax.fori_loop(0, 32, pull, 0)
    with jax.named_scope("leaf"):
        loads[4].wait()
        for l in range(ROWS // LEAF):
            at = slice(l * LEAF, (l + 1) * LEAF)
            field[:, at] = dot_nt(x[at, :].T[:VECS].astype(BF16), inverse[l])
    with jax.named_scope("gram_z"):

        @pl.when(core == 1)
        def _():
            share(1, g_b, send_g, recv_g, wait=True)
            zsum = (g_b[0, :96, :128].astype(F32) + g_b[1, :96, :128].astype(F32)) + (
                g_b[2, :96, :128].astype(F32) + g_b[3, :96, :128].astype(F32)
            )
            g_c[group(2)[1]] = zsum.astype(BF16)
            share(2, g_c, send_g, recv_g)

    with jax.named_scope("local"):
        vs = [
            dot_nt(
                field[:, b * LEAF : (b + 1) * LEAF].astype(BF16),
                right[:, :, b * LEAF : (b + 1) * LEAF].reshape(LEVELS * RANK, LEAF),
            )
            for b in range(16)
        ]
        for k in range(LOCAL):
            rest = (LEVELS - 1 - k) * RANK
            merged = []
            for m in range(len(vs) // 2):
                va, vb = vs[2 * m], vs[2 * m + 1]
                p2 = [
                    (v[:, rest : rest + RANK] * (1.0 / math.sqrt(LEAF * 2**k))).astype(BF16) for v in (vb, va)
                ]
                first = 32 - 2 ** (5 - k) + 2 * m
                g2 = jnp.concatenate([g_l[first, :, :rest], g_l[first + 1, :, :rest]], axis=0)
                merged.append(va[:, :rest] + vb[:, :rest] - dot(jnp.concatenate(p2, axis=1), g2))
                for n in range(2):
                    for b in range((2 * m + n) * 2**k, (2 * m + n + 1) * 2**k):
                        near[b, :, k * RANK : (k + 1) * RANK] = p2[n]
            vs = merged
        v = vs[0]

    def level_rows(k, g):
        if k == 1:
            return jnp.concatenate([g[128:160], g[160:]], axis=1)[:, above(1)]
        return g[rows_of(k), above(k)]

    def merge(k, va, vb, ga, gb):
        pa = (vb[:, block(k)] * scale[k]).astype(BF16)
        pb = (va[:, block(k)] * scale[k]).astype(BF16)
        if k == CROSS - 1:
            return pa, pb, None
        p2 = jnp.concatenate([pa, pb], axis=1)
        g2 = jnp.concatenate([level_rows(k, ga), level_rows(k, gb)], axis=0).astype(BF16)
        return pa, pb, va[:, above(k)] + vb[:, above(k)] - dot(p2, g2)

    with jax.named_scope("cross_core"):
        partner[:, 6 * RANK :] = jnp.zeros((VECS, 256 - 6 * RANK), BF16)
        v_a[core, :, 192:] = jnp.zeros((VECS, 64), F32)
        v_a[core, :, : CROSS * RANK] = v
        share(0, v_a, send_v, recv_v)
        share(0, v_a, send_v, recv_v, wait=True)
        mine = (v_a[1 - core, :, block(0)] * scale[0]).astype(BF16)

    def near_update():
        for b in range(16):
            at = slice(b * LEAF, (b + 1) * LEAF)
            field[:, at] -= dot(near[b], left[:LOCAL, :, at].reshape(LOCAL * RANK, LEAF)) + dot(
                mine, left[LOCAL, :, at]
            )

    def four(phase, k, v, v_buf, g_buf, meanwhile):
        me = group(phase)[1]
        if phase == 1:
            v_buf[me, :64] = v[:, :128].astype(BF16)
            v_buf[me, 64:] = fold(v[:, 128:]).astype(BF16)
        elif phase == 2:
            v_buf[me] = v.astype(BF16)
        else:
            v_buf[me] = fold(v).astype(BF16)
        share(phase, v_buf, send_v, recv_v)
        meanwhile()
        share(phase, v_buf, send_v, recv_v, wait=True)
        vs = [v_buf[i].astype(F32) for i in range(4)]
        if phase == 1:
            vs = [jnp.concatenate([u[:64], unfold(u[64:])], axis=1) for u in vs]
        elif phase == 3:
            vs = [unfold(u) for u in vs]
        gs = [g_buf[i].astype(F32) for i in range(4)]
        p0, p1, v01 = merge(k, vs[0], vs[1], gs[0], gs[1])
        p2, p3, v23 = merge(k, vs[2], vs[3], gs[2], gs[3])
        pa, pb, v = merge(k + 1, v01, v23, gs[0] + gs[1], gs[2] + gs[3])

        def keep():
            partner[:, (k - 1) * RANK : k * RANK] = jnp.where(
                me < 2, jnp.where(me == 0, p0, p1), jnp.where(me == 2, p2, p3)
            )
            partner[:, k * RANK : (k + 1) * RANK] = jnp.where(me < 2, pa, pb)

        return v, keep

    hand = remote(
        partner,
        partner,
        part_sem.at[0],
        part_sem.at[1],
        {"leaf": lax.axis_index("leaf"), "sub": lax.axis_index("sub") // 2 * 2},
    )
    with jax.named_scope("cross"):

        @pl.when(core == 1)
        def _():
            def first():
                share(2, g_c, send_g, recv_g, wait=True)
                xsum = (g_c[0, :32].astype(F32) + g_c[1, :32].astype(F32)) + (
                    g_c[2, :32].astype(F32) + g_c[3, :32].astype(F32)
                )
                g_d[group(3)[1]] = xsum.astype(BF16)
                share(3, g_d, send_g, recv_g)
                near_update()

            def last():
                keep()
                share(3, g_d, send_g, recv_g, wait=True)

            v = merge(0, v_a[0], v_a[1], g_a[0], g_a[1])[2]
            v, keep = four(1, 1, v, v_b, g_b, first)
            v, keep = four(2, 3, v, v_c, g_c, keep)
            v, keep = four(3, 5, v, v_d, g_d, last)
            keep()
            hand.start()
            hand.wait_send()

        @pl.when(core == 0)
        def _():
            near_update()
            hand.wait_recv()

    with jax.named_scope("finish"):
        for c in range(16):
            at = slice(c * LEAF, (c + 1) * LEAF)
            done = field[:, at] - dot(
                partner[:, : 6 * RANK], left[LOCAL + 1 :, :, at].reshape(6 * RANK, LEAF)
            )
            x[at, :] = jnp.concatenate([done, done], axis=0).T
        back_copy.wait()
        sent(src1, send_sem.at[0])
    with jax.named_scope("send_back"):
        gather_and_send(back, x, stage, src2, dst2, send_sem.at[1], recv2, -1)
    with jax.named_scope("receive_back"):
        flat_copy.wait()
        receive(dst2, recv2, y)
    with jax.named_scope("output"):
        alive = jnp.where(live_slots(counts, slots_ref[...]), 1, 0)

        slots_ref[...] = alive

        def pull_slots(a):
            for u in range(128):
                x[pl.ds(pl.multiple_of(a * 128, 128) + u, 1), :] = y[pl.ds(flat.at[u][a], 1), :]

        def push(a):
            at = pl.multiple_of(a * 128, 128)
            part = x[pl.ds(at, 128), :].T[:VECS]
            out[:, pl.ds(at, 128)] = jnp.where(slots_ref[pl.ds(a, 1), :] > 0, part, 0.0).astype(BF16)

        pull_slots(0)
        pull_slots(1)

        def next_slots(c, carry):
            push(2 * c)
            push(2 * c + 1)
            pull_slots(2 * c + 2)
            pull_slots(2 * c + 3)
            return carry

        lax.fori_loop(0, 19, next_slots, 0)
        push(38)
        push(39)
        sent(src2, send_sem.at[1])


def body(vectors, row_counts, tree_slot, leaf_inverse, left_basis, right_basis):
    outside = pl.BlockSpec(memory_space=pltpu.HBM)
    dma = pltpu.SemaphoreType.DMA
    blocks = pltpu.VMEM((DEV * 5, 4, 128), BF16)
    return pl.pallas_call(
        kernel,
        out_shape=jax.ShapeDtypeStruct((VECS, SLOTS), BF16),
        in_specs=[SMEM] + [outside] * 6,
        out_specs=VMEM,
        scratch_shapes=[
            pltpu.VMEM((DEV, 128), I32),
            pltpu.VMEM((40, 128), I32),
            pltpu.VMEM((VECS, SLOTS), BF16),
            pltpu.VMEM(leaf_inverse.shape, BF16),
            pltpu.VMEM(left_basis.shape, BF16),
            pltpu.VMEM(right_basis.shape, BF16),
            pltpu.VMEM((PEER, DEV), I32),
            pltpu.SMEM((PEER, DEV), I32),
            pltpu.VMEM((40, 128), F32),
            pltpu.VMEM((DEV, 128), I32),
            pltpu.SMEM((DEV, 128), I32),
            pltpu.VMEM((SLOTS, 128), F32),
            pltpu.VMEM((8, BLOCK, 128), F32),
            pltpu.VMEM((DEV, 1, 128), F32),
            pltpu.VMEM((DEV, 1, 128), F32),
            blocks,
            blocks,
            blocks,
            blocks,
            pltpu.VMEM((2 * DEV * BLOCK, 128), F32),
            pltpu.VMEM((64, 128), I32),
            pltpu.SMEM((64, 128), I32),
            pltpu.VMEM((PEER, DEV), I32),
            pltpu.SMEM((PEER, DEV), I32),
            pltpu.VMEM((VECS, ROWS), F32),
            pltpu.VMEM((2, VECS, 256), F32),
            pltpu.VMEM((4, 96, 128), BF16),
            pltpu.VMEM((4, VECS, 128), BF16),
            pltpu.VMEM((4, 32, 128), BF16),
            pltpu.VMEM((2, 192, 256), BF16),
            pltpu.VMEM((4, 192, 128), BF16),
            pltpu.VMEM((4, 96, 128), BF16),
            pltpu.VMEM((4, 32, 128), BF16),
            pltpu.VMEM((VECS, 256), BF16),
            pltpu.VMEM((30, RANK, 384), BF16),
            pltpu.VMEM((16, VECS, LOCAL * RANK), BF16),
            dma((6,)),
            dma((2,)),
            dma((2,)),
            dma((4,)),
            dma((2,)),
            dma((16,)),
            dma((16,)),
            dma((4,)),
            dma((4,)),
            dma((4,)),
            dma((4,)),
        ],
        compiler_params=pltpu.CompilerParams(
            collective_id=0, has_side_effects=True, vmem_limit_bytes=36 * 2**20
        ),
        name="apply",
    )(
        *(
            pltpu.with_memory_space_constraint(value, pltpu.HBM)
            for value in (
                row_counts,
                jnp.asarray(np.repeat(CODES[:, None], 128, 1)),
                tree_slot.reshape(40, 128),
                vectors,
                leaf_inverse,
                left_basis,
                right_basis,
            )
        ),
    )


def solution(mesh):
    both = ("leaf", "sub")
    return jax.shard_map(
        body,
        mesh=mesh,
        in_specs=(
            P(None, both),
            P(),
            P(both),
            P(both, None, None),
            P(None, None, both),
            P(None, None, both),
        ),
        out_specs=P(None, both),
        check_vma=False,
    )
```
